32 devices in a mesh: section: 2 (over y), dp: 16 (over z, x, core).
Axes of the slice: x: 2, y: 2, z: 4, core: 2. Of those that a mesh axis runs over, the one named last changes fastest.
Arguments:
- inputs: bfloat16 [32, 128, 1536], P('dp'), parts along dimension 0, may hold values from -6 to 6
- w_query: bfloat16 [2, 1536, 768], P('section'), may hold values from -0.15625 to 0.15625
- w_key: bfloat16 [2, 1536, 768], P('section'), may hold values from -0.15625 to 0.15625
- w_value: bfloat16 [2, 1536, 768], P('section'), may hold values from -0.15625 to 0.15625
- w_out: bfloat16 [2, 768, 1536], P('section'), may hold values from -0.21875 to 0.21875
- mixing: float32 [2], P('section'), may hold values from 0.2 to 0.8
Outputs:
- outputs: bfloat16 [32, 128, 1536], P(('dp', 'section')), parts along dimension 0
The draws below stay inside these ranges and needn't reach their ends.
There are 16 independent parts, one for each index of `dp`. The reference program is written for one: setup_inputs(seed, part) draws one part's arguments, and reference() takes and returns one part's arrays. A program takes and returns all parts, laid end to end along the dimension named above; an argument that names none is the same for every part. Nothing has to cross between parts.
All inputs are finite; a program needn't handle non-finite values.
Results may differ from the reference program's by a relative error of at most 0.023.
Values may be sent and summed in bfloat16 or wider, within the bound.
A program may use at most 128 MiB of HBM per device.

```python
import jax
import jax.numpy as jnp
from jax import lax

D = 1536
HEADS = 6
HEAD_DIM = 128
SEQ = 128
HD = 768
MICRO = 2
LAYERS = 2


def level_of(stream_key, dims, split, low, top_value):
    def one(position, shards_of):
        draws = jax.random.uniform(jax.random.fold_in(jax.random.fold_in(stream_key, 6), position), (shards_of,), jnp.float32, low / len(split), top_value / len(split))
        return jnp.repeat(jnp.exp(draws), dims[position] // shards_of).reshape((-1,) + (1,) * (len(dims) - position - 1))

    gain = one(*split[0])
    for cut in split[1:]:
        gain = gain * one(*cut)
    return gain


def scatter_about(key, dims, width, reach, pieces=(), kind=jnp.bfloat16):
    entries = jax.random.normal(key, dims, jnp.float32) * width
    if len(pieces) > 0:
        entries = level_of(key, dims, pieces, -0.22, 0.18) * entries
    return jnp.clip(entries, min=-reach, max=reach).astype(kind)


def setup_inputs(seed: int = 0, part: int = 0) -> dict:
    key_of = jax.random.split(jax.random.key(seed), 7)
    part_keys = jax.random.split(jax.random.fold_in(key_of[6], part), 7)
    inputs = scatter_about(part_keys[0], (MICRO, SEQ, D), 1.0, 6.0)
    w_query = scatter_about(key_of[1], (LAYERS, D, HD), D ** -0.5, 0.15625, ((0, 2),))
    w_key = scatter_about(key_of[2], (LAYERS, D, HD), D ** -0.5, 0.15625, ((0, 2),))
    w_value = scatter_about(key_of[3], (LAYERS, D, HD), D ** -0.5, 0.15625, ((0, 2),))
    w_out = scatter_about(key_of[4], (LAYERS, HD, D), HD ** -0.5, 0.21875, ((0, 2),))
    mixing = jnp.clip(0.2 + 0.6 * jax.random.uniform(key_of[5], (LAYERS,), jnp.float32) ** level_of(key_of[5], (LAYERS,), ((0, 2),), -0.2, 0.2), 0.2, 0.8)
    return dict(inputs=inputs, w_query=w_query, w_key=w_key, w_value=w_value, w_out=w_out, mixing=mixing)


epsilon = 1e-06
score_scale = 0.12

def norm_rows(tensor):
    return tensor * lax.rsqrt(lax.optimization_barrier(jnp.mean(tensor * tensor, axis=-1, keepdims=True)) + epsilon)

def layer_apply(hidden, w_query, w_key, w_value, w_out, mixing, first_values, first_flag):
    row_count = hidden.shape[0]
    hidden_wide = hidden.astype(jnp.float32)
    normed = norm_rows(hidden_wide).astype(jnp.bfloat16)
    queries = jnp.dot(normed, w_query, preferred_element_type=jnp.float32).reshape(row_count, HEADS, HEAD_DIM)
    key_rows = jnp.dot(normed, w_key, preferred_element_type=jnp.float32).reshape(row_count, HEADS, HEAD_DIM)
    queries = norm_rows(queries).astype(jnp.bfloat16)
    key_rows = norm_rows(key_rows).astype(jnp.bfloat16)
    values = jnp.dot(normed, w_value, preferred_element_type=jnp.float32)
    own_values = values.astype(jnp.bfloat16)
    if first_flag:
        used_values = own_values
    else:
        used_values = (mixing * values + (1.0 - mixing) * first_values.astype(jnp.float32)).astype(jnp.bfloat16)
    used_values = used_values.reshape(row_count, HEADS, HEAD_DIM)
    scores = jnp.einsum('qhd,khd->hqk', queries.astype(jnp.float32), key_rows.astype(jnp.float32)) * score_scale
    positions = jnp.arange(row_count, dtype=jnp.int32)
    causal = positions[:, None] >= positions[None, :]
    weights = jnp.where(causal[None, :, :], jnp.exp(scores), 0.0)
    probabilities = (weights / lax.optimization_barrier(jnp.sum(weights, axis=-1, keepdims=True))).astype(jnp.bfloat16)
    attended = jnp.einsum('hqk,khd->qhd', probabilities.astype(jnp.float32), used_values.astype(jnp.float32))
    attended = attended.astype(jnp.bfloat16).reshape(row_count, HEADS * HEAD_DIM)
    result = (hidden_wide + jnp.dot(attended, w_out, preferred_element_type=jnp.float32)).astype(jnp.bfloat16)
    return (result, own_values)

def reference(inputs, w_query, w_key, w_value, w_out, mixing):
    finished = []
    for micro_index in range(inputs.shape[0]):
        hidden = inputs[micro_index]
        first_values = None
        for layer_number in range(w_query.shape[0]):
            hidden, own_values = layer_apply(hidden, w_query[layer_number], w_key[layer_number], w_value[layer_number], w_out[layer_number], mixing[layer_number], first_values, layer_number == 0)
            if layer_number == 0:
                first_values = own_values
        finished.append(hidden)
    return jnp.stack(finished)
```

```python
import functools

import jax
import jax.numpy as jnp
from jax import lax
from jax.experimental import pallas as pl
from jax.experimental.pallas import tpu as pltpu
from jax.sharding import PartitionSpec as P

HEADS = 6

epsilon = 1e-06
score_scale = 0.12
MESH = pl.DeviceIdType.MESH


def norm_rows(tensor):
    return tensor * lax.rsqrt(jnp.mean(tensor * tensor, axis=-1, keepdims=True) + epsilon)


def project(normed, weight):
    return jnp.dot(normed, weight, preferred_element_type=jnp.float32)


def kernel(
    sections,
    inputs_ref,
    wq_hbm,
    wk_hbm,
    wv_hbm,
    wo_hbm,
    mixing_ref,
    out_ref,
    wq,
    wk,
    wv,
    wo,
    h_in,
    h_out,
    v_buf,
    q_buf,
    k_buf,
    val_buf,
    p_buf,
    att_buf,
    acc_buf,
    in_sem,
    wv_sem,
    load_sem,
    hs_sem,
    hr_sem,
    vs_sem,
    vr_sem,
    os_sem,
    or_sem,
):
    me = lax.axis_index("section")
    last = sections - 1
    micro, rows, width = h_in.shape
    features = v_buf.shape[2]
    head = features // HEADS
    chunks = HEADS // 2
    span = features // chunks
    share = micro // sections
    is_first = me == 0
    is_last = me == last
    bf16 = jnp.bfloat16
    f32 = jnp.float32

    def head_part(n):
        return slice(n * head, (n + 1) * head)

    def chunk_part(j):
        return slice(j * span, (j + 1) * span)

    def input_load(i):
        return pltpu.make_async_copy(inputs_ref.at[i], h_in.at[i], in_sem.at[i])

    def value_load(j):
        return pltpu.make_async_copy(
            wv_hbm.at[0, :, chunk_part(j)], wv.at[:, chunk_part(j)], wv_sem.at[j]
        )

    loads = [
        pltpu.make_async_copy(source.at[0], target, load_sem.at[i])
        for i, (source, target) in enumerate(((wq_hbm, wq), (wk_hbm, wk), (wo_hbm, wo)))
    ]

    barrier = pltpu.get_barrier_semaphore()
    for step in range(1, sections):
        pl.semaphore_signal(
            barrier,
            inc=1,
            device_id={"section": lax.rem(me + step, sections)},
            device_id_type=MESH,
        )

    @pl.when(is_first)
    def _():
        input_load(0).start()

    for j in range(chunks):
        value_load(j).start()
    for load in loads:
        load.start()

    @pl.when(is_first)
    def _():
        for i in range(1, micro):
            input_load(i).start()

    pl.semaphore_wait(barrier, sections - 1)

    onward = jnp.minimum(me + 1, last)

    def h_copy(i):
        return pltpu.make_async_remote_copy(
            src_ref=h_out.at[i],
            dst_ref=h_in.at[i],
            send_sem=hs_sem.at[i],
            recv_sem=hr_sem.at[i],
            device_id={"section": onward},
            device_id_type=MESH,
        )

    def v_copy(i, j):
        return pltpu.make_async_remote_copy(
            src_ref=v_buf.at[i, :, chunk_part(j)],
            dst_ref=v_buf.at[i, :, chunk_part(j)],
            send_sem=vs_sem.at[i, j],
            recv_sem=vr_sem.at[i, j],
            device_id={"section": onward},
            device_id_type=MESH,
        )

    def out_copy(i):
        return pltpu.make_async_remote_copy(
            src_ref=h_out.at[i],
            dst_ref=out_ref.at[i % share],
            send_sem=os_sem.at[i],
            recv_sem=or_sem.at[i],
            device_id={"section": i // share},
            device_id_type=MESH,
        )

    row_index = lax.broadcasted_iota(jnp.int32, (rows, rows), 0)
    column_index = lax.broadcasted_iota(jnp.int32, (rows, rows), 1)
    causal = row_index >= column_index

    def fill_probabilities(normed):
        queries = project(normed, wq[...])
        key_rows = project(normed, wk[...])
        for n in range(HEADS):
            q_buf[:, head_part(n)] = norm_rows(queries[:, head_part(n)]).astype(bf16)
            k_buf[:, head_part(n)] = norm_rows(key_rows[:, head_part(n)]).astype(bf16)
        for n in range(HEADS):
            scores = (
                lax.dot_general(
                    q_buf[:, head_part(n)],
                    k_buf[:, head_part(n)],
                    (((1,), (1,)), ((), ())),
                    preferred_element_type=f32,
                )
                * score_scale
            )
            weights = jnp.where(causal, jnp.exp(scores), 0.0)
            p_buf[n] = (weights / jnp.sum(weights, axis=-1, keepdims=True)).astype(bf16)

    @pl.when(is_first)
    def _():
        def one(i, carry):
            input_load(i).wait()
            normed = norm_rows(h_in[i].astype(f32)).astype(bf16)
            for j in range(chunks):

                @pl.when(i == 0)
                def _():
                    value_load(j).wait()

                v_buf[i, :, chunk_part(j)] = project(normed, wv[:, chunk_part(j)]).astype(bf16)
                if sections > 1:

                    @pl.when(i == 0)
                    def _():
                        v_copy(i, j).start()

            @pl.when(i == 0)
            def _():
                for load in loads:
                    load.wait()

            fill_probabilities(normed)
            for n in range(HEADS):
                att_buf[:, head_part(n)] = project(p_buf[n], v_buf[i, :, head_part(n)]).astype(bf16)
            result = (h_in[i].astype(f32) + project(att_buf[...], wo[...])).astype(bf16)
            if sections > 1:
                h_out[i] = result
                h_copy(i).start()

                @pl.when(i > 0)
                def _():
                    for j in range(chunks):
                        v_copy(i, j).start()

            else:
                out_ref[i] = result
            return carry

        lax.fori_loop(0, micro, one, 0)

    if sections > 1:

        @pl.when(jnp.logical_not(is_first))
        def _():
            for j in range(chunks):
                value_load(j).wait()
            for load in loads:
                load.wait()
            mixing = mixing_ref[0]

            def one(i, carry):
                h_copy(i).wait_recv()
                normed = norm_rows(h_in[i].astype(f32)).astype(bf16)
                fill_probabilities(normed)
                val_buf[...] = mixing * project(normed, wv[...])
                for j in range(chunks):
                    v_copy(i, j).wait_recv()
                    if sections > 2:

                        @pl.when(jnp.logical_not(is_last))
                        def _():
                            v_copy(i, j).start()

                    used = (
                        val_buf[:, chunk_part(j)]
                        + (1.0 - mixing) * v_buf[i, :, chunk_part(j)].astype(f32)
                    ).astype(bf16)
                    for n in range(2):
                        att_buf[:, head_part(2 * j + n)] = project(
                            p_buf[2 * j + n], used[:, head_part(n)]
                        ).astype(bf16)
                    term = project(att_buf[:, chunk_part(j)], wo[chunk_part(j), :])
                    if j == 0:
                        acc_buf[...] = term
                    elif j < chunks - 1:
                        acc_buf[...] += term
                result = (h_in[i].astype(f32) + (acc_buf[...] + term)).astype(bf16)
                mine = jnp.logical_and(is_last, i // share == last)

                @pl.when(mine)
                def _():
                    out_ref[i % share] = result

                @pl.when(jnp.logical_not(mine))
                def _():
                    h_out[i] = result

                    @pl.when(is_last)
                    def _():
                        out_copy(i).start()

                    if sections > 2:

                        @pl.when(jnp.logical_not(is_last))
                        def _():
                            h_copy(i).start()

                return carry

            lax.fori_loop(0, micro, one, 0)

    @pl.when(jnp.logical_not(is_last))
    def _():
        for i in range(micro):
            for j in range(chunks):
                v_copy(i, j).wait_send()
            h_copy(i).wait_send()

    for i in range(micro):
        if i // share != last:

            @pl.when(is_last)
            def _():
                out_copy(i).wait_send()

            @pl.when(me == i // share)
            def _():
                out_copy(i).wait_recv()


def body(inputs, w_query, w_key, w_value, w_out, mixing):
    sections = lax.axis_size("section")
    micro, rows, width = inputs.shape
    features = w_value.shape[2]
    share = micro // sections
    bf16 = jnp.bfloat16
    anywhere = pl.BlockSpec(memory_space=pltpu.HBM)
    dma = pltpu.SemaphoreType.DMA
    return pl.pallas_call(
        functools.partial(kernel, sections),
        out_shape=pltpu.VMEM((share, rows, width), bf16),
        in_specs=[anywhere] * 5 + [pl.BlockSpec(memory_space=pltpu.SMEM)],
        out_specs=pl.BlockSpec(memory_space=pltpu.VMEM),
        scratch_shapes=[
            pltpu.VMEM((width, features), bf16),
            pltpu.VMEM((width, features), bf16),
            pltpu.VMEM((width, features), bf16),
            pltpu.VMEM((features, width), bf16),
            pltpu.VMEM((micro, rows, width), bf16),
            pltpu.VMEM((micro, rows, width), bf16),
            pltpu.VMEM((micro, rows, features), bf16),
            pltpu.VMEM((rows, features), bf16),
            pltpu.VMEM((rows, features), bf16),
            pltpu.VMEM((rows, features), jnp.float32),
            pltpu.VMEM((HEADS, rows, rows), bf16),
            pltpu.VMEM((rows, features), bf16),
            pltpu.VMEM((rows, width), jnp.float32),
            dma((micro,)),
            dma((HEADS // 2,)),
            dma((3,)),
            dma((micro,)),
            dma((micro,)),
            dma((micro, HEADS // 2)),
            dma((micro, HEADS // 2)),
            dma((micro,)),
            dma((micro,)),
        ],
        compiler_params=pltpu.CompilerParams(
            collective_id=0, has_side_effects=True, vmem_limit_bytes=62 * 1024 * 1024
        ),
        name="sections",
    )(inputs, w_query, w_key, w_value, w_out, mixing)


def pair_kernel(
    inputs_ref,
    wq_hbm,
    wk_hbm,
    wv_hbm,
    wo_hbm,
    mixing_ref,
    out_ref,
    wq,
    wk,
    wv,
    wo,
    wx,
    h_in,
    h_out,
    normed_buf,
    v_buf,
    q_buf,
    k_buf,
    used_buf,
    p_buf,
    ps_buf,
    pv_buf,
    att_buf,
    q_acc,
    k_acc,
    v_acc,
    out_acc,
    in_sem,
    wv_sem,
    load_sem,
    hs_sem,
    hr_sem,
    cs_sem,
    cr_sem,
    vs_sem,
    vr_sem,
    ps_sem,
    pr_sem,
    ys_sem,
    yr_sem,
    xs_sem,
    xr_sem,
    ds_sem,
    dr_sem,
):
    me = lax.axis_index("section")
    dp = lax.axis_index("dp")
    across = dp + 2 - 4 * ((dp // 2) % 2)
    beside = dp + 1 - 2 * (dp % 2)
    quarter = dp % 4
    far_quarter = quarter + 2 - 4 * (quarter // 2)
    beside_quarters = beside % 4, far_quarter + 1 - 2 * (quarter % 2)
    micro, rows, width = h_in.shape
    features = wv.shape[1]
    head = features // HEADS
    chunks = HEADS // 2
    span = features // chunks
    cuts = cr_sem.shape[0]
    cut = width // cuts
    halves = hr_sem.shape[0]
    half = rows // halves
    pieces = yr_sem.shape[0]
    piece = features // (4 * pieces)
    bf16 = jnp.bfloat16
    f32 = jnp.float32

    def head_part(n):
        return slice(n * head, (n + 1) * head)

    def chunk_part(j):
        return slice(j * span, (j + 1) * span)

    def cut_part(c):
        return slice(c * cut, (c + 1) * cut)

    def half_part(t):
        return slice(t * half, (t + 1) * half)

    def input_load(i):
        return pltpu.make_async_copy(inputs_ref.at[i], h_in.at[i], in_sem.at[i])

    def value_load(j):
        return pltpu.make_async_copy(
            wv_hbm.at[0, :, chunk_part(j)], wv.at[:, chunk_part(j)], wv_sem.at[j]
        )

    query_load, key_load, out_load = (
        pltpu.make_async_copy(source.at[0], target, load_sem.at[i])
        for i, (source, target) in enumerate(((wq_hbm, wq), (wk_hbm, wk), (wo_hbm, wo)))
    )

    def send(source, target, send_sem, recv_sem, device):
        return pltpu.make_async_remote_copy(
            src_ref=source,
            dst_ref=target,
            send_sem=send_sem,
            recv_sem=recv_sem,
            device_id=device,
            device_id_type=MESH,
        )

    def half_copy(t):
        return send(
            h_out.at[0, half_part(t), :],
            h_in.at[0, half_part(t), :],
            hs_sem.at[t],
            hr_sem.at[t],
            {"section": 1},
        )

    def cut_copy(c):
        return send(
            h_out.at[1, :, cut_part(c)],
            h_in.at[1, :, cut_part(c)],
            cs_sem.at[c],
            cr_sem.at[c],
            {"section": 1},
        )

    def v_copy(j):
        part = v_buf.at[1, :, chunk_part(j)]
        return send(part, part, vs_sem.at[j], vr_sem.at[j], {"section": 1})

    def p_copy(t):
        part = ps_buf.at[:, half_part(t), :]
        return send(part, part, ps_sem.at[0, t], pr_sem.at[0, t], {"section": 0})

    def pv_copy(t):
        part = pv_buf.at[half_part(t), :]
        return send(part, part, ps_sem.at[1, t], pr_sem.at[1, t], {"section": 0})

    def piece_part(owner, i):
        return pl.ds(pl.multiple_of((owner * pieces + i) * piece, piece), piece)

    def y_copy(i):
        part = piece_part(quarter, i)
        return send(wo.at[part, :], wx.at[part, :], ys_sem.at[i], yr_sem.at[i], {"section": 0})

    def x_copy(owner, i):
        part = wx.at[piece_part(owner, i), :]
        return send(part, part, xs_sem.at[i], xr_sem.at[i], {"dp": across})

    def core_copy(far, owner, i):
        part = wx.at[piece_part(owner, i), :]
        return send(part, part, ds_sem.at[far, i], dr_sem.at[far, i], {"dp": beside})

    barrier = pltpu.get_barrier_semaphore()
    for device in ({"section": 1 - me}, {"dp": across}, {"dp": beside}):
        pl.semaphore_signal(barrier, inc=1, device_id=device, device_id_type=MESH)

    row_index = lax.broadcasted_iota(jnp.int32, (rows, rows), 0)
    column_index = lax.broadcasted_iota(jnp.int32, (rows, rows), 1)
    causal = row_index >= column_index

    def scores_of(part, keys, n):
        return (
            lax.dot_general(
                q_buf[part, head_part(n)],
                k_buf[:keys, head_part(n)],
                (((1,), (1,)), ((), ())),
                preferred_element_type=f32,
            )
            * score_scale
        )

    def fill_probabilities():
        for n in range(HEADS):
            weights = jnp.where(causal, jnp.exp(scores_of(slice(0, rows), rows, n)), 0.0)
            p_buf[n] = (weights / jnp.sum(weights, axis=-1, keepdims=True)).astype(bf16)

    def fill_heads(target, part, values):
        for n in range(HEADS):
            target[part, head_part(n)] = norm_rows(values[:, head_part(n)]).astype(bf16)

    @pl.when(me == 0)
    def _():
        for i in range(micro):
            input_load(i).start()
        for j in range(chunks):
            value_load(j).start()
        query_load.start()
        key_load.start()
        out_load.start()
        for i in range(micro):
            input_load(i).wait()
            normed_buf[i * rows : (i + 1) * rows, :] = norm_rows(h_in[i].astype(f32)).astype(bf16)
        pl.semaphore_wait(barrier, 3)
        for j in range(chunks):
            value_load(j).wait()
            values = project(normed_buf[...], wv[:, chunk_part(j)]).astype(bf16)
            v_buf[1, :, chunk_part(j)] = values[rows:, :]
            if j < chunks - 1:
                v_copy(j).start()
            v_buf[0, :, chunk_part(j)] = values[:rows, :]

        def attend(i):
            part = slice(i * rows, (i + 1) * rows)
            if i == 0:
                query_load.wait()
            fill_heads(q_buf, slice(0, rows), project(normed_buf[part, :], wq[...]))
            if i == 0:
                key_load.wait()
            fill_heads(k_buf, slice(0, rows), project(normed_buf[part, :], wk[...]))
            fill_probabilities()
            for n in range(HEADS):
                att_buf[:, head_part(n)] = project(p_buf[n], v_buf[i, :, head_part(n)]).astype(bf16)

        def pass_on(i):
            y_copy(i).wait_recv()
            x_copy(quarter, i).start()
            core_copy(0, quarter, i).start()

        def pass_far(i):
            x_copy(far_quarter, i).wait_recv()
            core_copy(1, far_quarter, i).start()

        attend(0)
        out_load.wait()
        for t in range(halves):
            h_out[0, half_part(t), :] = (
                h_in[0, half_part(t), :].astype(f32) + project(att_buf[half_part(t), :], wo[...])
            ).astype(bf16)
            half_copy(t).start()
        pass_on(0)
        attend(1)
        pass_on(1)
        for c in range(cuts):
            h_out[1, :, cut_part(c)] = (
                h_in[1, :, cut_part(c)].astype(f32) + project(att_buf[...], wo[:, cut_part(c)])
            ).astype(bf16)
            cut_copy(c).start()
        v_copy(chunks - 1).start()
        for i in range(2, pieces):
            pass_on(i)
            pass_far(i - 2)
        for i in range(pieces - 2, pieces):
            pass_far(i)
        for far in range(2):
            for i in range(pieces):
                core_copy(far, beside_quarters[far], i).wait_recv()
        for t in range(halves):
            keys = (t + 1) * half
            p_copy(t).wait_recv()
            pv_copy(t).wait_recv()
            for n in range(HEADS):
                att_buf[half_part(t), head_part(n)] = (
                    pv_buf[half_part(t), head_part(n)].astype(f32)
                    + project(ps_buf[n, half_part(t), :keys], v_buf[0, :keys, head_part(n)])
                ).astype(bf16)
            out_ref[0, half_part(t), :] = (
                h_out[0, half_part(t), :].astype(f32) + project(att_buf[half_part(t), :], wx[...])
            ).astype(bf16)
        for t in range(halves):
            half_copy(t).wait_send()
        for c in range(cuts):
            cut_copy(c).wait_send()
        for j in range(chunks):
            v_copy(j).wait_send()
        for i in range(pieces):
            x_copy(quarter, i).wait_send()
            core_copy(0, quarter, i).wait_send()
            core_copy(1, far_quarter, i).wait_send()

    @pl.when(me == 1)
    def _():
        out_load.start()
        query_load.start()
        key_load.start()
        for j in range(chunks):
            value_load(j).start()
        mixing = mixing_ref[0]
        ps_buf[...] = jnp.zeros_like(ps_buf)
        out_load.wait()
        pl.semaphore_wait(barrier, 3)
        for i in range(pieces):
            y_copy(i).start()
        query_load.wait()
        key_load.wait()
        for j in range(chunks):
            value_load(j).wait()
        for t in range(halves):
            part = half_part(t)
            keys = (t + 1) * half
            half_copy(t).wait_recv()
            normed = norm_rows(h_in[0, part, :].astype(f32)).astype(bf16)
            fill_heads(q_buf, part, project(normed, wq[...]))
            fill_heads(k_buf, part, project(normed, wk[...]))
            used_buf[part, :] = (mixing * project(normed, wv[...])).astype(bf16)
            for n in range(HEADS):
                weights = jnp.where(causal[part, :keys], jnp.exp(scores_of(part, keys, n)), 0.0)
                share = weights / jnp.sum(weights, axis=-1, keepdims=True)
                ps_buf[n, part, :keys] = ((1.0 - mixing) * share).astype(bf16)
                pv_buf[part, head_part(n)] = project(
                    share.astype(bf16), used_buf[:keys, head_part(n)]
                ).astype(bf16)
            p_copy(t).start()
            pv_copy(t).start()
        squares = jnp.zeros((rows, 1), f32)
        for c in range(cuts):
            cut_copy(c).wait_recv()
            piece_in = h_in[1, :, cut_part(c)]
            for target, weight in ((q_acc, wq), (k_acc, wk), (v_acc, wv)):
                term = project(piece_in, weight[cut_part(c), :])
                if c == 0:
                    target[...] = term
                else:
                    target[...] += term
            wide = piece_in.astype(f32)
            squares += jnp.sum(wide * wide, axis=-1, keepdims=True)
        scale = lax.rsqrt(squares / width + epsilon)
        fill_heads(q_buf, slice(0, rows), q_acc[...] * scale)
        fill_heads(k_buf, slice(0, rows), k_acc[...] * scale)
        fill_probabilities()
        for j in range(chunks):
            v_copy(j).wait_recv()
            used = (
                mixing * (v_acc[:, chunk_part(j)] * scale)
                + (1.0 - mixing) * v_buf[1, :, chunk_part(j)].astype(f32)
            ).astype(bf16)
            for n in range(2):
                att_buf[:, head_part(2 * j + n)] = project(
                    p_buf[2 * j + n], used[:, head_part(n)]
                ).astype(bf16)
            term = project(att_buf[:, chunk_part(j)], wo[chunk_part(j), :])
            if j == 0:
                out_acc[...] = term
            elif j < chunks - 1:
                out_acc[...] += term
        out_ref[0] = (h_in[1].astype(f32) + (out_acc[...] + term)).astype(bf16)
        for i in range(pieces):
            y_copy(i).wait_send()
        for t in range(halves):
            p_copy(t).wait_send()
            pv_copy(t).wait_send()


def pair_body(inputs, w_query, w_key, w_value, w_out, mixing):
    micro, rows, width = inputs.shape
    features = w_value.shape[2]
    head = features // HEADS
    chunks = HEADS // 2
    halves, cuts, pieces = 2, 6, 6
    bf16 = jnp.bfloat16
    f32 = jnp.float32
    anywhere = pl.BlockSpec(memory_space=pltpu.HBM)
    dma = pltpu.SemaphoreType.DMA
    return pl.pallas_call(
        pair_kernel,
        out_shape=pltpu.VMEM((1, rows, width), bf16),
        in_specs=[anywhere] * 5 + [pl.BlockSpec(memory_space=pltpu.SMEM)],
        out_specs=pl.BlockSpec(memory_space=pltpu.VMEM),
        scratch_shapes=[
            pltpu.VMEM((width, features), bf16),
            pltpu.VMEM((width, features), bf16),
            pltpu.VMEM((width, features), bf16),
            pltpu.VMEM((features, width), bf16),
            pltpu.VMEM((features, width), bf16),
            pltpu.VMEM((micro, rows, width), bf16),
            pltpu.VMEM((micro, rows, width), bf16),
            pltpu.VMEM((micro * rows, width), bf16),
            pltpu.VMEM((micro, rows, features), bf16),
            pltpu.VMEM((rows, features), bf16),
            pltpu.VMEM((rows, features), bf16),
            pltpu.VMEM((rows, features), bf16),
            pltpu.VMEM((HEADS, rows, rows), bf16),
            pltpu.VMEM((HEADS, rows, rows), bf16),
            pltpu.VMEM((rows, features), bf16),
            pltpu.VMEM((rows, features), bf16),
            pltpu.VMEM((rows, features), f32),
            pltpu.VMEM((rows, features), f32),
            pltpu.VMEM((rows, features), f32),
            pltpu.VMEM((rows, width), f32),
            dma((micro,)),
            dma((chunks,)),
            dma((3,)),
            dma((halves,)),
            dma((halves,)),
            dma((cuts,)),
            dma((cuts,)),
            dma((chunks,)),
            dma((chunks,)),
            dma((2, halves)),
            dma((2, halves)),
            dma((pieces,)),
            dma((pieces,)),
            dma((pieces,)),
            dma((pieces,)),
            dma((2, pieces)),
            dma((2, pieces)),
        ],
        compiler_params=pltpu.CompilerParams(
            collective_id=0, has_side_effects=True, vmem_limit_bytes=62 * 1024 * 1024
        ),
        name="section_pair",
    )(inputs, w_query, w_key, w_value, w_out, mixing)


def solution(mesh):
    in_specs = (
        P("dp", None, None),
        P("section", None, None),
        P("section", None, None),
        P("section", None, None),
        P("section", None, None),
        P("section"),
    )
    out_specs = P(("dp", "section"), None, None)
    paired = mesh.shape["section"] == 2 and mesh.shape["dp"] % 4 == 0

    def either(inputs, *weights):
        chosen = pair_body if paired and inputs.shape[0] == 2 else body
        return chosen(inputs, *weights)

    return jax.shard_map(either, mesh=mesh, in_specs=in_specs, out_specs=out_specs, check_vma=False)
```

```python
import functools

import jax
import jax.numpy as jnp
from jax import lax
from jax.experimental import pallas as pl
from jax.experimental.pallas import tpu as pltpu
from jax.sharding import PartitionSpec as P

HEADS = 6
CUTS = 6
PIECES = 4

epsilon = 1e-06
score_scale = 0.12
MESH = pl.DeviceIdType.MESH


def norm_rows(tensor):
    return tensor * lax.rsqrt(jnp.mean(tensor * tensor, axis=-1, keepdims=True) + epsilon)


def project(normed, weight):
    return jnp.dot(normed, weight, preferred_element_type=jnp.float32)


def kernel(
    sections,
    inputs_ref,
    wq_hbm,
    wk_hbm,
    wv_hbm,
    wo_hbm,
    mixing_ref,
    out_ref,
    wq,
    wk,
    wv,
    wo,
    h_in,
    h_out,
    v_buf,
    q_buf,
    k_buf,
    val_buf,
    p_buf,
    att_buf,
    acc_buf,
    in_sem,
    wv_sem,
    load_sem,
    hs_sem,
    hr_sem,
    vs_sem,
    vr_sem,
    os_sem,
    or_sem,
):
    me = lax.axis_index("section")
    last = sections - 1
    micro, rows, width = h_in.shape
    features = v_buf.shape[2]
    head = features // HEADS
    chunks = HEADS // 2
    span = features // chunks
    share = micro // sections
    is_first = me == 0
    is_last = me == last
    bf16 = jnp.bfloat16
    f32 = jnp.float32

    def head_part(n):
        return slice(n * head, (n + 1) * head)

    def chunk_part(j):
        return slice(j * span, (j + 1) * span)

    def input_load(i):
        return pltpu.make_async_copy(inputs_ref.at[i], h_in.at[i], in_sem.at[i])

    def value_load(j):
        return pltpu.make_async_copy(
            wv_hbm.at[0, :, chunk_part(j)], wv.at[:, chunk_part(j)], wv_sem.at[j]
        )

    loads = [
        pltpu.make_async_copy(source.at[0], target, load_sem.at[i])
        for i, (source, target) in enumerate(((wq_hbm, wq), (wk_hbm, wk), (wo_hbm, wo)))
    ]

    barrier = pltpu.get_barrier_semaphore()
    for step in range(1, sections):
        pl.semaphore_signal(
            barrier,
            inc=1,
            device_id={"section": lax.rem(me + step, sections)},
            device_id_type=MESH,
        )

    @pl.when(is_first)
    def _():
        input_load(0).start()

    for j in range(chunks):
        value_load(j).start()
    for load in loads:
        load.start()

    @pl.when(is_first)
    def _():
        for i in range(1, micro):
            input_load(i).start()

    pl.semaphore_wait(barrier, sections - 1)

    onward = jnp.minimum(me + 1, last)

    def h_copy(i):
        return pltpu.make_async_remote_copy(
            src_ref=h_out.at[i],
            dst_ref=h_in.at[i],
            send_sem=hs_sem.at[i],
            recv_sem=hr_sem.at[i],
            device_id={"section": onward},
            device_id_type=MESH,
        )

    def v_copy(i, j):
        return pltpu.make_async_remote_copy(
            src_ref=v_buf.at[i, :, chunk_part(j)],
            dst_ref=v_buf.at[i, :, chunk_part(j)],
            send_sem=vs_sem.at[i, j],
            recv_sem=vr_sem.at[i, j],
            device_id={"section": onward},
            device_id_type=MESH,
        )

    def out_copy(i):
        return pltpu.make_async_remote_copy(
            src_ref=h_out.at[i],
            dst_ref=out_ref.at[i % share],
            send_sem=os_sem.at[i],
            recv_sem=or_sem.at[i],
            device_id={"section": i // share},
            device_id_type=MESH,
        )

    row_index = lax.broadcasted_iota(jnp.int32, (rows, rows), 0)
    column_index = lax.broadcasted_iota(jnp.int32, (rows, rows), 1)
    causal = row_index >= column_index

    def fill_probabilities(normed):
        queries = project(normed, wq[...])
        key_rows = project(normed, wk[...])
        for n in range(HEADS):
            q_buf[:, head_part(n)] = norm_rows(queries[:, head_part(n)]).astype(bf16)
            k_buf[:, head_part(n)] = norm_rows(key_rows[:, head_part(n)]).astype(bf16)
        for n in range(HEADS):
            scores = (
                lax.dot_general(
                    q_buf[:, head_part(n)],
                    k_buf[:, head_part(n)],
                    (((1,), (1,)), ((), ())),
                    preferred_element_type=f32,
                )
                * score_scale
            )
            weights = jnp.where(causal, jnp.exp(scores), 0.0)
            p_buf[n] = (weights / jnp.sum(weights, axis=-1, keepdims=True)).astype(bf16)

    @pl.when(is_first)
    def _():
        def one(i, carry):
            input_load(i).wait()
            normed = norm_rows(h_in[i].astype(f32)).astype(bf16)
            for j in range(chunks):

                @pl.when(i == 0)
                def _():
                    value_load(j).wait()

                v_buf[i, :, chunk_part(j)] = project(normed, wv[:, chunk_part(j)]).astype(bf16)
                if sections > 1:

                    @pl.when(i == 0)
                    def _():
                        v_copy(i, j).start()

            @pl.when(i == 0)
            def _():
                for load in loads:
                    load.wait()

            fill_probabilities(normed)
            for n in range(HEADS):
                att_buf[:, head_part(n)] = project(p_buf[n], v_buf[i, :, head_part(n)]).astype(bf16)
            result = (h_in[i].astype(f32) + project(att_buf[...], wo[...])).astype(bf16)
            if sections > 1:
                h_out[i] = result
                h_copy(i).start()

                @pl.when(i > 0)
                def _():
                    for j in range(chunks):
                        v_copy(i, j).start()

            else:
                out_ref[i] = result
            return carry

        lax.fori_loop(0, micro, one, 0)

    if sections > 1:

        @pl.when(jnp.logical_not(is_first))
        def _():
            for j in range(chunks):
                value_load(j).wait()
            for load in loads:
                load.wait()
            mixing = mixing_ref[0]

            def one(i, carry):
                h_copy(i).wait_recv()
                normed = norm_rows(h_in[i].astype(f32)).astype(bf16)
                fill_probabilities(normed)
                val_buf[...] = mixing * project(normed, wv[...])
                for j in range(chunks):
                    v_copy(i, j).wait_recv()
                    if sections > 2:

                        @pl.when(jnp.logical_not(is_last))
                        def _():
                            v_copy(i, j).start()

                    used = (
                        val_buf[:, chunk_part(j)]
                        + (1.0 - mixing) * v_buf[i, :, chunk_part(j)].astype(f32)
                    ).astype(bf16)
                    for n in range(2):
                        att_buf[:, head_part(2 * j + n)] = project(
                            p_buf[2 * j + n], used[:, head_part(n)]
                        ).astype(bf16)
                    term = project(att_buf[:, chunk_part(j)], wo[chunk_part(j), :])
                    if j == 0:
                        acc_buf[...] = term
                    elif j < chunks - 1:
                        acc_buf[...] += term
                result = (h_in[i].astype(f32) + (acc_buf[...] + term)).astype(bf16)
                mine = jnp.logical_and(is_last, i // share == last)

                @pl.when(mine)
                def _():
                    out_ref[i % share] = result

                @pl.when(jnp.logical_not(mine))
                def _():
                    h_out[i] = result

                    @pl.when(is_last)
                    def _():
                        out_copy(i).start()

                    if sections > 2:

                        @pl.when(jnp.logical_not(is_last))
                        def _():
                            h_copy(i).start()

                return carry

            lax.fori_loop(0, micro, one, 0)

    @pl.when(jnp.logical_not(is_last))
    def _():
        for i in range(micro):
            for j in range(chunks):
                v_copy(i, j).wait_send()
            h_copy(i).wait_send()

    for i in range(micro):
        if i // share != last:

            @pl.when(is_last)
            def _():
                out_copy(i).wait_send()

            @pl.when(me == i // share)
            def _():
                out_copy(i).wait_recv()


def body(inputs, w_query, w_key, w_value, w_out, mixing):
    sections = lax.axis_size("section")
    micro, rows, width = inputs.shape
    features = w_value.shape[2]
    share = micro // sections
    bf16 = jnp.bfloat16
    anywhere = pl.BlockSpec(memory_space=pltpu.HBM)
    dma = pltpu.SemaphoreType.DMA
    return pl.pallas_call(
        functools.partial(kernel, sections),
        out_shape=pltpu.VMEM((share, rows, width), bf16),
        in_specs=[anywhere] * 5 + [pl.BlockSpec(memory_space=pltpu.SMEM)],
        out_specs=pl.BlockSpec(memory_space=pltpu.VMEM),
        scratch_shapes=[
            pltpu.VMEM((width, features), bf16),
            pltpu.VMEM((width, features), bf16),
            pltpu.VMEM((width, features), bf16),
            pltpu.VMEM((features, width), bf16),
            pltpu.VMEM((micro, rows, width), bf16),
            pltpu.VMEM((micro, rows, width), bf16),
            pltpu.VMEM((micro, rows, features), bf16),
            pltpu.VMEM((rows, features), bf16),
            pltpu.VMEM((rows, features), bf16),
            pltpu.VMEM((rows, features), jnp.float32),
            pltpu.VMEM((HEADS, rows, rows), bf16),
            pltpu.VMEM((rows, features), bf16),
            pltpu.VMEM((rows, width), jnp.float32),
            dma((micro,)),
            dma((HEADS // 2,)),
            dma((3,)),
            dma((micro,)),
            dma((micro,)),
            dma((micro, HEADS // 2)),
            dma((micro, HEADS // 2)),
            dma((micro,)),
            dma((micro,)),
        ],
        compiler_params=pltpu.CompilerParams(
            collective_id=0, has_side_effects=True, vmem_limit_bytes=62 * 1024 * 1024
        ),
        name="sections",
    )(inputs, w_query, w_key, w_value, w_out, mixing)


def pair_kernel(
    inputs_ref,
    wq_hbm,
    wk_hbm,
    wv_hbm,
    wo_hbm,
    mixing_ref,
    out_ref,
    wq,
    wk,
    wv,
    wo,
    wx,
    h_in,
    h_out,
    normed_buf,
    v_buf,
    q_buf,
    k_buf,
    used_buf,
    p_buf,
    low_buf,
    high_buf,
    att_buf,
    q_acc,
    k_acc,
    v_acc,
    val_buf,
    out_acc,
    load_sem,
    send_sem,
    recv_sem,
    met_sem,
):
    me = lax.axis_index("section")
    dp = lax.axis_index("dp")
    core = dp % 2
    across = dp + 2 - 4 * ((dp // 2) % 2)
    along = dp + 4 - 8 * ((dp // 4) % 2)
    beside = dp + 1 - 2 * core
    quarter = (dp // 2 + dp // 4) % 2 * 2 + core
    far_quarter = quarter + 2 - 4 * (quarter // 2)
    micro, rows, width = h_in.shape
    features = wv.shape[1]
    head = features // HEADS
    chunks = HEADS // 2
    span = features // chunks
    half = rows // 2
    cut = width // CUTS
    share = features // 4
    piece = share // PIECES
    bf16 = jnp.bfloat16
    f32 = jnp.float32
    everything = slice(0, rows)
    early = slice(0, (chunks - 1) * span)
    late = slice((chunks - 1) * span, features)

    def head_part(n):
        return slice(n * head, (n + 1) * head)

    def chunk_part(j):
        return slice(j * span, (j + 1) * span)

    def cut_part(c):
        return slice(c * cut, (c + 1) * cut)

    def half_part(t):
        return slice(t * half, (t + 1) * half)

    def sequence_part(i):
        return slice(i * rows, (i + 1) * rows)

    def load(source, target, n):
        return pltpu.make_async_copy(source, target, load_sem.at[n])

    def input_load(i):
        return load(inputs_ref.at[i], h_in.at[i], i)

    def value_load(j):
        return load(wv_hbm.at[0, :, chunk_part(j)], wv.at[:, chunk_part(j)], 2 + j)

    query_load = load(wq_hbm.at[0], wq, 5)
    key_load = load(wk_hbm.at[0], wk, 6)
    out_load = load(wo_hbm.at[0], wo, 7)
    values_load = load(wv_hbm.at[0], wv, 2)
    rest_load = load(wo_hbm.at[0, : 3 * share, :], wo.at[: 3 * share, :], 1)

    def share_load(r):
        part = pl.ds(pl.multiple_of((quarter + r) % 4 * share, share), share)
        return load(wo_hbm.at[0, part, :], wo.at[part, :], min(r, 1))

    def send(source, target, sent, received, device):
        return pltpu.make_async_remote_copy(
            src_ref=source,
            dst_ref=target,
            send_sem=send_sem.at[sent],
            recv_sem=recv_sem.at[received],
            device_id=device,
            device_id_type=MESH,
        )

    def half_copy(i, t):
        part = (i, half_part(t))
        return send(h_out.at[part], h_in.at[part], 0, 2 * i + t, {"section": 1})

    def cut_copy(c):
        part = (1, half_part(1), cut_part(c))
        return send(h_out.at[part], h_in.at[part], 0, 3 + c, {"section": 1})

    def v_copy(part, n):
        return send(v_buf.at[1, :, part], v_buf.at[1, :, part], 1, 3 + CUTS + n, {"section": 1})

    def low_copy():
        return send(low_buf, low_buf, 2, 0, {"section": 0})

    def high_copy(g):
        return send(high_buf.at[g], high_buf.at[g], 3, 1 + g, {"section": 0})

    def piece_part(owner, i):
        return pl.ds(pl.multiple_of(owner * share + i * piece, piece), piece)

    def y_copy(i):
        part = piece_part(quarter, i)
        return send(wo.at[part, :], wx.at[part, :], min(i, 1), 3 + i, {"section": 0})

    def side_copy(owner, i):
        part = wx.at[piece_part(owner, i), :]
        return send(part, part, 2, 3 + PIECES + i, {"dp": along if i % 2 else across})

    def core_copy(owner, i):
        part = wx.at[piece_part(owner, i), :]
        return send(part, part, 3, 3 + 2 * PIECES, {"dp": beside})

    def rows_wait(count, sent, received):
        part = wx.at[:count, :]
        return send(part, part, sent, received, {"dp": beside})

    barrier = pltpu.get_barrier_semaphore()

    @pl.when(me == 1)
    def _():
        share_load(0).start()
        pl.semaphore_wait(barrier, 1)
        pl.semaphore_signal(met_sem, inc=1, device_id={"section": 0}, device_id_type=MESH)

    @pl.when(me == 0)
    def _():
        for device in ({"section": 1}, {"dp": across}, {"dp": along}, {"dp": beside}):
            pl.semaphore_signal(barrier, inc=1, device_id=device, device_id_type=MESH)

    row_index = lax.broadcasted_iota(jnp.int32, (rows, rows), 0)
    column_index = lax.broadcasted_iota(jnp.int32, (rows, rows), 1)
    causal = row_index >= column_index

    def normed_rows(values):
        return norm_rows(values.astype(f32)).astype(bf16)

    def fill_heads(target, part, values):
        for n in range(HEADS):
            target[part, head_part(n)] = norm_rows(values[:, head_part(n)]).astype(bf16)

    def probabilities(part, keys, n):
        scores = (
            lax.dot_general(
                q_buf[part, head_part(n)],
                k_buf[:keys, head_part(n)],
                (((1,), (1,)), ((), ())),
                preferred_element_type=f32,
            )
            * score_scale
        )
        weights = jnp.where(causal[part, :keys], jnp.exp(scores), 0.0)
        return weights / jnp.sum(weights, axis=-1, keepdims=True)

    @pl.when(me == 0)
    def _():
        input_load(1).start()
        value_load(0).start()
        input_load(0).start()
        for j in range(1, chunks):
            value_load(j).start()

        def fill_normed(i):
            with jax.named_scope(f"in{i}"):
                input_load(i).wait()
            normed_buf[sequence_part(i), :] = normed_rows(h_in[i])

        def fill_values(i, j):
            v_buf[i, :, chunk_part(j)] = project(
                normed_buf[sequence_part(i), :], wv[:, chunk_part(j)]
            ).astype(bf16)

        fill_normed(1)
        query_load.start()
        key_load.start()
        out_load.start()
        for j in range(chunks):
            with jax.named_scope(f"wv{j}"):
                value_load(j).wait()
            fill_values(1, j)
            if j == 0:
                with jax.named_scope("met"):
                    pl.semaphore_wait(met_sem, 1)
            if j < chunks - 1:
                v_copy(chunk_part(j), 0).start()
            else:

                @pl.when(core == 0)
                def _():
                    v_copy(late, 1).start()

        fill_normed(0)
        for j in range(chunks):
            fill_values(0, j)

        def attend(i):
            normed = normed_buf[sequence_part(i), :]
            if i == 0:
                with jax.named_scope("wq"):
                    query_load.wait()
            fill_heads(q_buf, everything, project(normed, wq[...]))
            if i == 0:
                with jax.named_scope("wk"):
                    key_load.wait()
            fill_heads(k_buf, everything, project(normed, wk[...]))
            for n in range(HEADS):
                p_buf[n] = probabilities(everything, rows, n).astype(bf16)
            for n in range(HEADS):
                att_buf[:, head_part(n)] = project(p_buf[n], v_buf[i, :, head_part(n)]).astype(bf16)

        def next_rows(i, part, columns):
            h_out[i, part, columns] = (
                h_in[i, part, columns].astype(f32) + project(att_buf[part, :], wo[:, columns])
            ).astype(bf16)

        def pass_on(i):
            with jax.named_scope(f"pass{i}"):
                y_copy(i).wait_recv()
            side_copy(quarter, i).start()
            core_copy(quarter, i).start()

        def pass_far(i):
            with jax.named_scope(f"far{i}"):
                side_copy(far_quarter, i).wait_recv()
            core_copy(far_quarter, i).start()

        attend(0)
        with jax.named_scope("wo"):
            out_load.wait()
        for t in range(2):
            with jax.named_scope(f"h0{t}"):
                next_rows(0, half_part(t), slice(0, width))
                half_copy(0, t).start()
        with jax.named_scope("bar"):
            pl.semaphore_wait(barrier, 3)
        pass_on(0)
        attend(1)
        with jax.named_scope("h1"):
            next_rows(1, half_part(0), slice(0, width))
            half_copy(1, 0).start()
            for c in range(CUTS):
                next_rows(1, half_part(1), cut_part(c))
                cut_copy(c).start()

        @pl.when(core == 1)
        def _():
            v_copy(late, 1).start()

        for i in range(1, PIECES):
            pass_on(i)
            pass_far(i - 1)
        pass_far(PIECES - 1)
        with jax.named_scope("core"):
            rows_wait(2 * share, 3, 3 + 2 * PIECES).wait_recv()
        for t in range(2):
            part = half_part(t)
            keys = (t + 1) * half
            for n in range(HEADS):
                group, place = n // chunks, n % chunks
                if t == 0:
                    if n == 0:
                        with jax.named_scope("low"):
                            low_copy().wait_recv()
                    passed = low_buf[n // 2, :, n % 2 * half : (n % 2 + 1) * half]
                    own = low_buf[chunks + n]
                else:
                    if place == 0:
                        with jax.named_scope(f"high{group}"):
                            high_copy(group).wait_recv()
                    passed = high_buf[group, place]
                    own = high_buf[group, chunks + place]
                att_buf[part, head_part(n)] = (
                    own.astype(f32) + project(passed, v_buf[0, :keys, head_part(n)])
                ).astype(bf16)
            out_ref[0, part, :] = (
                h_out[0, part, :].astype(f32) + project(att_buf[part, :], wx[...])
            ).astype(bf16)
        with jax.named_scope("end"):
            send(h_out, h_in, 0, 0, {"section": 1}).wait_send()
            send(v_buf.at[1], v_buf.at[1], 1, 0, {"section": 1}).wait_send()
            rows_wait(share, 2, 0).wait_send()
            rows_wait(2 * share, 3, 0).wait_send()

    @pl.when(me == 1)
    def _():
        mixing = mixing_ref[0]
        with jax.named_scope("wo"):
            share_load(0).wait()
        for i in range(PIECES):
            y_copy(i).start()
        with jax.named_scope("y0"):
            rows_wait(piece, 0, 0).wait_send()
        query_load.start()
        key_load.start()
        values_load.start()
        for r in range(1, 4):
            share_load(r).start()
        with jax.named_scope("loads"):
            query_load.wait()
            key_load.wait()
            values_load.wait()
            rest_load.wait()

        def fill_rows(i, t):
            part = half_part(t)
            with jax.named_scope(f"half{i}{t}"):
                half_copy(i, t).wait_recv()
            normed = normed_rows(h_in[i, part, :])
            fill_heads(q_buf, part, project(normed, wq[...]))
            fill_heads(k_buf, part, project(normed, wk[...]))
            return mixing * project(normed, wv[...])

        for t in range(2):
            part = half_part(t)
            keys = (t + 1) * half
            used_buf[part, :] = fill_rows(0, t).astype(bf16)
            for n in range(HEADS):
                group, place = n // chunks, n % chunks
                shares = probabilities(part, keys, n)
                passed = ((1.0 - mixing) * shares).astype(bf16)
                own = project(shares.astype(bf16), used_buf[:keys, head_part(n)]).astype(bf16)
                if t == 0:
                    low_buf[n // 2, :, n % 2 * half : (n % 2 + 1) * half] = passed
                    low_buf[chunks + n] = own
                else:
                    high_buf[group, place] = passed
                    high_buf[group, chunks + place] = own
                    if place == chunks - 1:
                        high_copy(group).start()
            if t == 0:
                low_copy().start()

        def fill_used(part, columns):
            used_buf[part, columns] = (
                val_buf[part, columns] + (1.0 - mixing) * v_buf[1, part, columns].astype(f32)
            ).astype(bf16)

        def fill_attended(t, heads):
            part = half_part(t)
            keys = (t + 1) * half
            for n in heads:
                att_buf[part, head_part(n)] = project(
                    p_buf[n, part, :keys], used_buf[:keys, head_part(n)]
                ).astype(bf16)

        def finish_rows(t):
            part = half_part(t)
            keys = (t + 1) * half
            for n in range(HEADS):
                p_buf[n, part, :keys] = probabilities(part, keys, n).astype(bf16)
            fill_used(part, early)
            fill_attended(t, range(HEADS - 2))
            out_acc[part, :] = h_in[1, part, :].astype(f32) + project(att_buf[part, early], wo[early, :])

        val_buf[half_part(0), :] = fill_rows(1, 0)
        with jax.named_scope("first0"):
            v_copy(early, 0).wait_recv()
        finish_rows(0)
        squares = jnp.zeros((half, 1), f32)
        for c in range(CUTS):
            with jax.named_scope(f"cut{c}"):
                cut_copy(c).wait_recv()
            arrived = h_in[1, half_part(1), cut_part(c)]
            for target, weight in ((q_acc, wq), (k_acc, wk), (v_acc, wv)):
                term = project(arrived, weight[cut_part(c), :])
                if c == 0:
                    target[...] = term
                else:
                    target[...] += term
            wide = arrived.astype(f32)
            squares += jnp.sum(wide * wide, axis=-1, keepdims=True)
        with jax.named_scope("last"):
            scale = lax.rsqrt(squares / width + epsilon)
            fill_heads(q_buf, half_part(1), q_acc[...] * scale)
            fill_heads(k_buf, half_part(1), k_acc[...] * scale)
            val_buf[half_part(1), :] = mixing * (v_acc[...] * scale)
            finish_rows(1)
        with jax.named_scope("first1"):
            v_copy(late, 1).wait_recv()
        with jax.named_scope("out"):
            fill_used(everything, late)
            for t in range(2):
                fill_attended(t, range(HEADS - 2, HEADS))
            out_ref[0] = (out_acc[...] + project(att_buf[:, late], wo[late, :])).astype(bf16)
        with jax.named_scope("end"):
            rows_wait(share - piece, 1, 0).wait_send()
            send(low_buf, low_buf, 2, 0, {"section": 0}).wait_send()
            send(high_buf, high_buf, 3, 0, {"section": 0}).wait_send()


def pair_body(inputs, w_query, w_key, w_value, w_out, mixing):
    micro, rows, width = inputs.shape
    features = w_value.shape[2]
    half = rows // 2
    chunks = HEADS // 2
    head = features // HEADS
    bf16 = jnp.bfloat16
    f32 = jnp.float32
    anywhere = pl.BlockSpec(memory_space=pltpu.HBM)
    dma = pltpu.SemaphoreType.DMA
    return pl.pallas_call(
        pair_kernel,
        out_shape=pltpu.VMEM((1, rows, width), bf16),
        in_specs=[anywhere] * 5 + [pl.BlockSpec(memory_space=pltpu.SMEM)],
        out_specs=pl.BlockSpec(memory_space=pltpu.VMEM),
        scratch_shapes=[
            pltpu.VMEM((width, features), bf16),
            pltpu.VMEM((width, features), bf16),
            pltpu.VMEM((width, features), bf16),
            pltpu.VMEM((features, width), bf16),
            pltpu.VMEM((features, width), bf16),
            pltpu.VMEM((micro, rows, width), bf16),
            pltpu.VMEM((micro, rows, width), bf16),
            pltpu.VMEM((micro * rows, width), bf16),
            pltpu.VMEM((micro, rows, features), bf16),
            pltpu.VMEM((rows, features), bf16),
            pltpu.VMEM((rows, features), bf16),
            pltpu.VMEM((rows, features), bf16),
            pltpu.VMEM((HEADS, rows, rows), bf16),
            pltpu.VMEM((chunks + HEADS, half, head), bf16),
            pltpu.VMEM((2, HEADS, half, head), bf16),
            pltpu.VMEM((rows, features), bf16),
            pltpu.VMEM((half, features), f32),
            pltpu.VMEM((half, features), f32),
            pltpu.VMEM((half, features), f32),
            pltpu.VMEM((rows, features), f32),
            pltpu.VMEM((rows, width), f32),
            dma((8,)),
            dma((4,)),
            dma((max(5 + CUTS, 4 + 2 * PIECES),)),
            pltpu.SemaphoreType.REGULAR,
        ],
        compiler_params=pltpu.CompilerParams(
            collective_id=0, has_side_effects=True, vmem_limit_bytes=62 * 1024 * 1024
        ),
        name="section_pair",
    )(inputs, w_query, w_key, w_value, w_out, mixing)


def solution(mesh):
    in_specs = (
        P("dp", None, None),
        P("section", None, None),
        P("section", None, None),
        P("section", None, None),
        P("section", None, None),
        P("section"),
    )
    out_specs = P(("dp", "section"), None, None)
    paired = mesh.shape["section"] == 2 and mesh.shape["dp"] % 8 == 0

    def either(inputs, *weights):
        square = inputs.shape[1] * HEADS == weights[2].shape[2]
        chosen = pair_body if paired and square and inputs.shape[0] == 2 else body
        return chosen(inputs, *weights)

    return jax.shard_map(either, mesh=mesh, in_specs=in_specs, out_specs=out_specs, check_vma=False)
```

```python
import functools

import jax
import jax.numpy as jnp
from jax import lax
from jax.experimental import pallas as pl
from jax.experimental.pallas import tpu as pltpu
from jax.sharding import PartitionSpec as P

HEADS = 6
CUTS = ((3, 3), (3, 6))
PIECES = (3, 5)
HELD = 4

epsilon = 1e-06
score_scale = 0.12
MESH = pl.DeviceIdType.MESH


def norm_rows(tensor):
    return tensor * lax.rsqrt(jnp.mean(tensor * tensor, axis=-1, keepdims=True) + epsilon)


def project(normed, weight):
    return jnp.dot(normed, weight, preferred_element_type=jnp.float32)


def kernel(
    sections,
    inputs_ref,
    wq_hbm,
    wk_hbm,
    wv_hbm,
    wo_hbm,
    mixing_ref,
    out_ref,
    wq,
    wk,
    wv,
    wo,
    h_in,
    h_out,
    v_buf,
    q_buf,
    k_buf,
    val_buf,
    p_buf,
    att_buf,
    acc_buf,
    in_sem,
    wv_sem,
    load_sem,
    hs_sem,
    hr_sem,
    vs_sem,
    vr_sem,
    os_sem,
    or_sem,
):
    me = lax.axis_index("section")
    last = sections - 1
    micro, rows, width = h_in.shape
    features = v_buf.shape[2]
    head = features // HEADS
    chunks = HEADS // 2
    span = features // chunks
    share = micro // sections
    is_first = me == 0
    is_last = me == last
    bf16 = jnp.bfloat16
    f32 = jnp.float32

    def head_part(n):
        return slice(n * head, (n + 1) * head)

    def chunk_part(j):
        return slice(j * span, (j + 1) * span)

    def input_load(i):
        return pltpu.make_async_copy(inputs_ref.at[i], h_in.at[i], in_sem.at[i])

    def value_load(j):
        return pltpu.make_async_copy(
            wv_hbm.at[0, :, chunk_part(j)], wv.at[:, chunk_part(j)], wv_sem.at[j]
        )

    loads = [
        pltpu.make_async_copy(source.at[0], target, load_sem.at[i])
        for i, (source, target) in enumerate(((wq_hbm, wq), (wk_hbm, wk), (wo_hbm, wo)))
    ]

    barrier = pltpu.get_barrier_semaphore()
    for step in range(1, sections):
        pl.semaphore_signal(
            barrier,
            inc=1,
            device_id={"section": lax.rem(me + step, sections)},
            device_id_type=MESH,
        )

    @pl.when(is_first)
    def _():
        input_load(0).start()

    for j in range(chunks):
        value_load(j).start()
    for load in loads:
        load.start()

    @pl.when(is_first)
    def _():
        for i in range(1, micro):
            input_load(i).start()

    pl.semaphore_wait(barrier, sections - 1)

    onward = jnp.minimum(me + 1, last)

    def h_copy(i):
        return pltpu.make_async_remote_copy(
            src_ref=h_out.at[i],
            dst_ref=h_in.at[i],
            send_sem=hs_sem.at[i],
            recv_sem=hr_sem.at[i],
            device_id={"section": onward},
            device_id_type=MESH,
        )

    def v_copy(i, j):
        return pltpu.make_async_remote_copy(
            src_ref=v_buf.at[i, :, chunk_part(j)],
            dst_ref=v_buf.at[i, :, chunk_part(j)],
            send_sem=vs_sem.at[i, j],
            recv_sem=vr_sem.at[i, j],
            device_id={"section": onward},
            device_id_type=MESH,
        )

    def out_copy(i):
        return pltpu.make_async_remote_copy(
            src_ref=h_out.at[i],
            dst_ref=out_ref.at[i % share],
            send_sem=os_sem.at[i],
            recv_sem=or_sem.at[i],
            device_id={"section": i // share},
            device_id_type=MESH,
        )

    row_index = lax.broadcasted_iota(jnp.int32, (rows, rows), 0)
    column_index = lax.broadcasted_iota(jnp.int32, (rows, rows), 1)
    causal = row_index >= column_index

    def fill_probabilities(normed):
        queries = project(normed, wq[...])
        key_rows = project(normed, wk[...])
        for n in range(HEADS):
            q_buf[:, head_part(n)] = norm_rows(queries[:, head_part(n)]).astype(bf16)
            k_buf[:, head_part(n)] = norm_rows(key_rows[:, head_part(n)]).astype(bf16)
        for n in range(HEADS):
            scores = (
                lax.dot_general(
                    q_buf[:, head_part(n)],
                    k_buf[:, head_part(n)],
                    (((1,), (1,)), ((), ())),
                    preferred_element_type=f32,
                )
                * score_scale
            )
            weights = jnp.where(causal, jnp.exp(scores), 0.0)
            p_buf[n] = (weights / jnp.sum(weights, axis=-1, keepdims=True)).astype(bf16)

    @pl.when(is_first)
    def _():
        def one(i, carry):
            input_load(i).wait()
            normed = norm_rows(h_in[i].astype(f32)).astype(bf16)
            for j in range(chunks):

                @pl.when(i == 0)
                def _():
                    value_load(j).wait()

                v_buf[i, :, chunk_part(j)] = project(normed, wv[:, chunk_part(j)]).astype(bf16)
                if sections > 1:

                    @pl.when(i == 0)
                    def _():
                        v_copy(i, j).start()

            @pl.when(i == 0)
            def _():
                for load in loads:
                    load.wait()

            fill_probabilities(normed)
            for n in range(HEADS):
                att_buf[:, head_part(n)] = project(p_buf[n], v_buf[i, :, head_part(n)]).astype(bf16)
            result = (h_in[i].astype(f32) + project(att_buf[...], wo[...])).astype(bf16)
            if sections > 1:
                h_out[i] = result
                h_copy(i).start()

                @pl.when(i > 0)
                def _():
                    for j in range(chunks):
                        v_copy(i, j).start()

            else:
                out_ref[i] = result
            return carry

        lax.fori_loop(0, micro, one, 0)

    if sections > 1:

        @pl.when(jnp.logical_not(is_first))
        def _():
            for j in range(chunks):
                value_load(j).wait()
            for load in loads:
                load.wait()
            mixing = mixing_ref[0]

            def one(i, carry):
                h_copy(i).wait_recv()
                normed = norm_rows(h_in[i].astype(f32)).astype(bf16)
                fill_probabilities(normed)
                val_buf[...] = mixing * project(normed, wv[...])
                for j in range(chunks):
                    v_copy(i, j).wait_recv()
                    if sections > 2:

                        @pl.when(jnp.logical_not(is_last))
                        def _():
                            v_copy(i, j).start()

                    used = (
                        val_buf[:, chunk_part(j)]
                        + (1.0 - mixing) * v_buf[i, :, chunk_part(j)].astype(f32)
                    ).astype(bf16)
                    for n in range(2):
                        att_buf[:, head_part(2 * j + n)] = project(
                            p_buf[2 * j + n], used[:, head_part(n)]
                        ).astype(bf16)
                    term = project(att_buf[:, chunk_part(j)], wo[chunk_part(j), :])
                    if j == 0:
                        acc_buf[...] = term
                    elif j < chunks - 1:
                        acc_buf[...] += term
                result = (h_in[i].astype(f32) + (acc_buf[...] + term)).astype(bf16)
                mine = jnp.logical_and(is_last, i // share == last)

                @pl.when(mine)
                def _():
                    out_ref[i % share] = result

                @pl.when(jnp.logical_not(mine))
                def _():
                    h_out[i] = result

                    @pl.when(is_last)
                    def _():
                        out_copy(i).start()

                    if sections > 2:

                        @pl.when(jnp.logical_not(is_last))
                        def _():
                            h_copy(i).start()

                return carry

            lax.fori_loop(0, micro, one, 0)

    @pl.when(jnp.logical_not(is_last))
    def _():
        for i in range(micro):
            for j in range(chunks):
                v_copy(i, j).wait_send()
            h_copy(i).wait_send()

    for i in range(micro):
        if i // share != last:

            @pl.when(is_last)
            def _():
                out_copy(i).wait_send()

            @pl.when(me == i // share)
            def _():
                out_copy(i).wait_recv()


def body(inputs, w_query, w_key, w_value, w_out, mixing):
    sections = lax.axis_size("section")
    micro, rows, width = inputs.shape
    features = w_value.shape[2]
    share = micro // sections
    bf16 = jnp.bfloat16
    anywhere = pl.BlockSpec(memory_space=pltpu.HBM)
    dma = pltpu.SemaphoreType.DMA
    return pl.pallas_call(
        functools.partial(kernel, sections),
        out_shape=pltpu.VMEM((share, rows, width), bf16),
        in_specs=[anywhere] * 5 + [pl.BlockSpec(memory_space=pltpu.SMEM)],
        out_specs=pl.BlockSpec(memory_space=pltpu.VMEM),
        scratch_shapes=[
            pltpu.VMEM((width, features), bf16),
            pltpu.VMEM((width, features), bf16),
            pltpu.VMEM((width, features), bf16),
            pltpu.VMEM((features, width), bf16),
            pltpu.VMEM((micro, rows, width), bf16),
            pltpu.VMEM((micro, rows, width), bf16),
            pltpu.VMEM((micro, rows, features), bf16),
            pltpu.VMEM((rows, features), bf16),
            pltpu.VMEM((rows, features), bf16),
            pltpu.VMEM((rows, features), jnp.float32),
            pltpu.VMEM((HEADS, rows, rows), bf16),
            pltpu.VMEM((rows, features), bf16),
            pltpu.VMEM((rows, width), jnp.float32),
            dma((micro,)),
            dma((HEADS // 2,)),
            dma((3,)),
            dma((micro,)),
            dma((micro,)),
            dma((micro, HEADS // 2)),
            dma((micro, HEADS // 2)),
            dma((micro,)),
            dma((micro,)),
        ],
        compiler_params=pltpu.CompilerParams(
            collective_id=0, has_side_effects=True, vmem_limit_bytes=62 * 1024 * 1024
        ),
        name="sections",
    )(inputs, w_query, w_key, w_value, w_out, mixing)


def pair_kernel(
    inputs_ref,
    wq_hbm,
    wk_hbm,
    wv_hbm,
    wo_hbm,
    mixing_ref,
    out_ref,
    wq,
    wk,
    wv,
    wo,
    wx,
    h_in,
    h_out,
    normed_buf,
    v_buf,
    q_buf,
    k_buf,
    used_buf,
    p_buf,
    low_buf,
    high_buf,
    att_buf,
    q_acc,
    k_acc,
    v_acc,
    val_buf,
    out_acc,
    load_sem,
    send_sem,
    recv_sem,
    met_sem,
):
    me = lax.axis_index("section")
    dp = lax.axis_index("dp")
    core = dp % 2
    across = dp + 2 - 4 * ((dp // 2) % 2)
    along = dp + 4 - 8 * ((dp // 4) % 2)
    beside = dp + 1 - 2 * core
    near = (dp // 2 + dp // 4) % 2
    most = max(PIECES)
    micro, rows, width = h_in.shape
    features = wv.shape[1]
    head = features // HEADS
    chunks = HEADS // 2
    span = features // chunks
    half = rows // 2
    share = features // 2
    piece = share // sum(PIECES)
    bf16 = jnp.bfloat16
    f32 = jnp.float32
    everything = slice(0, rows)
    early = slice(0, (chunks - 1) * span)
    late = slice((chunks - 1) * span, features)

    def head_part(n):
        return slice(n * head, (n + 1) * head)

    def chunk_part(j):
        return slice(j * span, (j + 1) * span)

    def cut_parts(i, t):
        cut = width // CUTS[i][t]
        return [slice(c * cut, (c + 1) * cut) for c in range(CUTS[i][t])]

    def half_part(t):
        return slice(t * half, (t + 1) * half)

    def sequence_part(i):
        return slice(i * rows, (i + 1) * rows)

    def load(source, target, n):
        return pltpu.make_async_copy(source, target, load_sem.at[n])

    def input_load(i):
        return load(inputs_ref.at[i], h_in.at[i], i)

    def value_load(j):
        return load(wv_hbm.at[0, :, chunk_part(j)], wv.at[:, chunk_part(j)], 2 + j)

    query_load = load(wq_hbm.at[0], wq, 5)
    key_load = load(wk_hbm.at[0], wk, 6)
    out_load = load(wo_hbm.at[0], wo, 7)
    values_load = load(wv_hbm.at[0], wv, 2)

    def share_load(r):
        part = pl.ds(pl.multiple_of((near + r) % 2 * share, share), share)
        return load(wo_hbm.at[0, part, :], wo.at[part, :], r)

    def send(source, target, sent, received, device):
        return pltpu.make_async_remote_copy(
            src_ref=source,
            dst_ref=target,
            send_sem=send_sem.at[sent],
            recv_sem=recv_sem.at[received],
            device_id=device,
            device_id_type=MESH,
        )

    def cut_copy(i, t, c):
        part = (i, half_part(t), cut_parts(i, t)[c])
        place = sum((CUTS[0] + CUTS[1])[: 2 * i + t]) + c
        return send(h_out.at[part], h_in.at[part], 0, place, {"section": 1})

    def v_copy(part, n):
        return send(v_buf.at[1, :, part], v_buf.at[1, :, part], 1, sum(CUTS[0] + CUTS[1]) + n, {"section": 1})

    def low_copy():
        return send(low_buf, low_buf, 2, 0, {"section": 0})

    def high_copy(g):
        return send(high_buf.at[g], high_buf.at[g], 3, 1 + g, {"section": 0})

    def piece_part(far, i):
        start = (near + far) % 2 * share + core * PIECES[0] * piece + i * piece
        return pl.ds(pl.multiple_of(start, piece), piece)

    def y_copy(i):
        part = piece_part(0, i)
        return send(wo.at[part, :], wx.at[part, :], min(i, 1), 3 + i, {"section": 0})

    def side_copy(far, i):
        part = wx.at[piece_part(far, i), :]
        return send(part, part, 2, 3 + most + i, {"dp": along if i % 2 else across})

    def core_copy(far, i):
        part = wx.at[piece_part(far, i), :]
        return send(part, part, 3, 3 + 2 * most, {"dp": beside})

    def pieces_wait(count, sent, received):
        part = wx.at[: count * piece, :]
        return send(part, part, sent, received, {"dp": beside})

    def for_piece(i, run):
        if i < min(PIECES):
            run()
        else:
            pl.when(core == 1)(run)

    def for_core(run):
        for n in range(2):
            pl.when(core == n)(functools.partial(run, PIECES[n], PIECES[1 - n]))

    barrier = pltpu.get_barrier_semaphore()

    @pl.when(me == 1)
    def _():
        share_load(0).start()
        pl.semaphore_wait(barrier, 1)
        pl.semaphore_signal(met_sem, inc=1, device_id={"section": 0}, device_id_type=MESH)

    @pl.when(me == 0)
    def _():
        for device in ({"section": 1}, {"dp": across}, {"dp": along}, {"dp": beside}):
            pl.semaphore_signal(barrier, inc=1, device_id=device, device_id_type=MESH)

    row_index = lax.broadcasted_iota(jnp.int32, (rows, rows), 0)
    column_index = lax.broadcasted_iota(jnp.int32, (rows, rows), 1)
    causal = row_index >= column_index

    def normed_rows(values):
        return norm_rows(values.astype(f32)).astype(bf16)

    def fill_heads(target, part, values):
        for n in range(HEADS):
            target[part, head_part(n)] = norm_rows(values[:, head_part(n)]).astype(bf16)

    def probabilities(part, keys, n):
        scores = (
            lax.dot_general(
                q_buf[part, head_part(n)],
                k_buf[:keys, head_part(n)],
                (((1,), (1,)), ((), ())),
                preferred_element_type=f32,
            )
            * score_scale
        )
        weights = jnp.where(causal[part, :keys], jnp.exp(scores), 0.0)
        return weights / jnp.sum(weights, axis=-1, keepdims=True)

    @pl.when(me == 0)
    def _():
        input_load(1).start()
        value_load(0).start()
        input_load(0).start()
        for j in range(1, chunks):
            value_load(j).start()

        def fill_normed(i):
            with jax.named_scope(f"in{i}"):
                input_load(i).wait()
            normed_buf[sequence_part(i), :] = normed_rows(h_in[i])

        def fill_values(i, j):
            v_buf[i, :, chunk_part(j)] = project(
                normed_buf[sequence_part(i), :], wv[:, chunk_part(j)]
            ).astype(bf16)

        fill_normed(1)
        query_load.start()
        key_load.start()
        out_load.start()
        for j in range(chunks - 1):
            with jax.named_scope(f"wv{j}"):
                value_load(j).wait()
            fill_values(1, j)
            if j == 0:
                with jax.named_scope("met"):
                    pl.semaphore_wait(met_sem, 1)
            v_copy(chunk_part(j), 0).start()
        fill_normed(0)
        value_load(chunks - 1).wait()
        for j in range(chunks):
            fill_values(0, j)

        def fill_queries(i):
            normed = normed_buf[sequence_part(i), :]
            if i == 0:
                with jax.named_scope("wq"):
                    query_load.wait()
            fill_heads(q_buf, everything, project(normed, wq[...]))
            if i == 0:
                with jax.named_scope("wk"):
                    key_load.wait()
            fill_heads(k_buf, everything, project(normed, wk[...]))

        def attend(i, part, keys):
            for n in range(HEADS):
                p_buf[n, part, :keys] = probabilities(part, keys, n).astype(bf16)
            for n in range(HEADS):
                att_buf[part, head_part(n)] = project(
                    p_buf[n, part, :keys], v_buf[i, :keys, head_part(n)]
                ).astype(bf16)

        def next_rows(i, t):
            part = half_part(t)
            for c, columns in enumerate(cut_parts(i, t)):
                h_out[i, part, columns] = (
                    h_in[i, part, columns].astype(f32) + project(att_buf[part, :], wo[:, columns])
                ).astype(bf16)
                if (i, t) == (0, 0) or (i, t) == (1, 1) and c > HELD:
                    cut_copy(i, t, c).start()
                if (i, t, c) == (1, 1, HELD):
                    pl.when(core == 1)(functools.partial(start_rows, 0, 1))
                    start_rows(1, 0)
                    for earlier in range(c + 1):
                        cut_copy(i, t, earlier).start()

        def start_rows(i, t):
            for c in range(CUTS[i][t]):
                cut_copy(i, t, c).start()

        def pass_on(i):
            with jax.named_scope(f"pass{i}"):
                y_copy(i).wait_recv()
            side_copy(0, i).start()
            core_copy(0, i).start()

        def pass_far(i):
            with jax.named_scope(f"far{i}"):
                side_copy(1, i).wait_recv()
            core_copy(1, i).start()

        fill_queries(0)
        for t in range(2):
            attend(0, half_part(t), (t + 1) * half)
            if t == 0:
                with jax.named_scope("wo"):
                    out_load.wait()
            with jax.named_scope(f"h0{t}"):
                next_rows(0, t)
        pl.when(core == 0)(functools.partial(start_rows, 0, 1))
        fill_values(1, chunks - 1)
        with jax.named_scope("bar"):
            pl.semaphore_wait(barrier, 3)
        pass_on(0)
        fill_queries(1)
        attend(1, everything, rows)
        with jax.named_scope("h1"):
            for t in range(2):
                next_rows(1, t)
        v_copy(late, 1).start()
        for i in range(1, most):
            for_piece(i, functools.partial(pass_on, i))
            for_piece(i - 1, functools.partial(pass_far, i - 1))
        for_piece(most - 1, functools.partial(pass_far, most - 1))
        with jax.named_scope("core"):
            for_core(lambda own, other: pieces_wait(2 * other, 3, 3 + 2 * most).wait_recv())
        for t in range(2):
            part = half_part(t)
            keys = (t + 1) * half
            for n in range(HEADS):
                group, place = n // chunks, n % chunks
                if t == 0:
                    if n == 0:
                        with jax.named_scope("low"):
                            low_copy().wait_recv()
                    passed = low_buf[n // 2, :, n % 2 * half : (n % 2 + 1) * half]
                    own = low_buf[chunks + n]
                else:
                    if place == 0:
                        with jax.named_scope(f"high{group}"):
                            high_copy(group).wait_recv()
                    passed = high_buf[group, place]
                    own = high_buf[group, chunks + place]
                att_buf[part, head_part(n)] = (
                    own.astype(f32) + project(passed, v_buf[0, :keys, head_part(n)])
                ).astype(bf16)
            out_ref[0, part, :] = (
                h_out[0, part, :].astype(f32) + project(att_buf[part, :], wx[...])
            ).astype(bf16)
        with jax.named_scope("end"):
            send(h_out, h_in, 0, 0, {"section": 1}).wait_send()
            send(v_buf.at[1], v_buf.at[1], 1, 0, {"section": 1}).wait_send()
            for_core(lambda own, other: pieces_wait(own, 2, 0).wait_send())
            for_core(lambda own, other: pieces_wait(2 * own, 3, 0).wait_send())

    @pl.when(me == 1)
    def _():
        mixing = mixing_ref[0]
        with jax.named_scope("wo"):
            share_load(0).wait()
        for i in range(most):
            for_piece(i, lambda: y_copy(i).start())
        with jax.named_scope("y0"):
            pieces_wait(1, 0, 0).wait_send()
        query_load.start()
        key_load.start()
        values_load.start()
        share_load(1).start()
        with jax.named_scope("loads"):
            query_load.wait()
            key_load.wait()
            values_load.wait()
            share_load(1).wait()

        def fill_rows(i, t):
            part = half_part(t)
            squares = jnp.zeros((half, 1), f32)
            for c, columns in enumerate(cut_parts(i, t)):
                with jax.named_scope(f"cut{i}{t}{c}"):
                    cut_copy(i, t, c).wait_recv()
                arrived = h_in[i, part, columns]
                for target, weight in ((q_acc, wq), (k_acc, wk), (v_acc, wv)):
                    term = project(arrived, weight[columns, :])
                    if c == 0:
                        target[...] = term
                    else:
                        target[...] += term
                wide = arrived.astype(f32)
                squares += jnp.sum(wide * wide, axis=-1, keepdims=True)
            scale = lax.rsqrt(squares / width + epsilon)
            fill_heads(q_buf, part, q_acc[...] * scale)
            fill_heads(k_buf, part, k_acc[...] * scale)
            return mixing * (v_acc[...] * scale)

        for t in range(2):
            part = half_part(t)
            keys = (t + 1) * half
            used_buf[part, :] = fill_rows(0, t).astype(bf16)
            for n in range(HEADS):
                group, place = n // chunks, n % chunks
                shares = probabilities(part, keys, n)
                passed = ((1.0 - mixing) * shares).astype(bf16)
                own = project(shares.astype(bf16), used_buf[:keys, head_part(n)]).astype(bf16)
                if t == 0:
                    low_buf[n // 2, :, n % 2 * half : (n % 2 + 1) * half] = passed
                    low_buf[chunks + n] = own
                else:
                    high_buf[group, place] = passed
                    high_buf[group, chunks + place] = own
                    if place == chunks - 1:
                        high_copy(group).start()
            if t == 0:
                low_copy().start()

        def fill_used(part, columns):
            used_buf[part, columns] = (
                val_buf[part, columns] + (1.0 - mixing) * v_buf[1, part, columns].astype(f32)
            ).astype(bf16)

        def fill_attended(t, heads):
            part = half_part(t)
            keys = (t + 1) * half
            for n in heads:
                att_buf[part, head_part(n)] = project(
                    p_buf[n, part, :keys], used_buf[:keys, head_part(n)]
                ).astype(bf16)

        def finish_rows(t):
            part = half_part(t)
            keys = (t + 1) * half
            for n in range(HEADS):
                p_buf[n, part, :keys] = probabilities(part, keys, n).astype(bf16)
            fill_used(part, early)
            fill_attended(t, range(HEADS - 2))
            out_acc[part, :] = h_in[1, part, :].astype(f32) + project(
                att_buf[part, early], wo[early, :]
            )

        val_buf[half_part(0), :] = fill_rows(1, 0)
        v_copy(early, 0).wait_recv()
        finish_rows(0)
        val_buf[half_part(1), :] = fill_rows(1, 1)
        with jax.named_scope("last"):
            finish_rows(1)
        with jax.named_scope("first"):
            v_copy(late, 1).wait_recv()
        with jax.named_scope("out"):
            fill_used(everything, late)
            for t in range(2):
                fill_attended(t, range(HEADS - 2, HEADS))
            out_ref[0] = (out_acc[...] + project(att_buf[:, late], wo[late, :])).astype(bf16)
        with jax.named_scope("end"):
            for_core(lambda own, other: pieces_wait(own - 1, 1, 0).wait_send())
            send(low_buf, low_buf, 2, 0, {"section": 0}).wait_send()
            send(high_buf, high_buf, 3, 0, {"section": 0}).wait_send()


def pair_body(inputs, w_query, w_key, w_value, w_out, mixing):
    micro, rows, width = inputs.shape
    features = w_value.shape[2]
    half = rows // 2
    chunks = HEADS // 2
    head = features // HEADS
    bf16 = jnp.bfloat16
    f32 = jnp.float32
    anywhere = pl.BlockSpec(memory_space=pltpu.HBM)
    dma = pltpu.SemaphoreType.DMA
    return pl.pallas_call(
        pair_kernel,
        out_shape=pltpu.VMEM((1, rows, width), bf16),
        in_specs=[anywhere] * 5 + [pl.BlockSpec(memory_space=pltpu.SMEM)],
        out_specs=pl.BlockSpec(memory_space=pltpu.VMEM),
        scratch_shapes=[
            pltpu.VMEM((width, features), bf16),
            pltpu.VMEM((width, features), bf16),
            pltpu.VMEM((width, features), bf16),
            pltpu.VMEM((features, width), bf16),
            pltpu.VMEM((features, width), bf16),
            pltpu.VMEM((micro, rows, width), bf16),
            pltpu.VMEM((micro, rows, width), bf16),
            pltpu.VMEM((micro * rows, width), bf16),
            pltpu.VMEM((micro, rows, features), bf16),
            pltpu.VMEM((rows, features), bf16),
            pltpu.VMEM((rows, features), bf16),
            pltpu.VMEM((rows, features), bf16),
            pltpu.VMEM((HEADS, rows, rows), bf16),
            pltpu.VMEM((chunks + HEADS, half, head), bf16),
            pltpu.VMEM((2, HEADS, half, head), bf16),
            pltpu.VMEM((rows, features), bf16),
            pltpu.VMEM((half, features), f32),
            pltpu.VMEM((half, features), f32),
            pltpu.VMEM((half, features), f32),
            pltpu.VMEM((rows, features), f32),
            pltpu.VMEM((rows, width), f32),
            dma((8,)),
            dma((4,)),
            dma((max(2 + sum(CUTS[0] + CUTS[1]), 4 + 2 * max(PIECES)),)),
            pltpu.SemaphoreType.REGULAR,
        ],
        compiler_params=pltpu.CompilerParams(
            collective_id=0, has_side_effects=True, vmem_limit_bytes=62 * 1024 * 1024
        ),
        name="section_pair",
    )(inputs, w_query, w_key, w_value, w_out, mixing)


def solution(mesh):
    in_specs = (
        P("dp", None, None),
        P("section", None, None),
        P("section", None, None),
        P("section", None, None),
        P("section", None, None),
        P("section"),
    )
    out_specs = P(("dp", "section"), None, None)
    paired = mesh.shape["section"] == 2 and mesh.shape["dp"] % 8 == 0

    def either(inputs, *weights):
        square = inputs.shape[1] * HEADS == weights[2].shape[2]
        chosen = pair_body if paired and square and inputs.shape[0] == 2 else body
        return chosen(inputs, *weights)

    return jax.shard_map(either, mesh=mesh, in_specs=in_specs, out_specs=out_specs, check_vma=False)
```

```python
import functools

import jax
import jax.numpy as jnp
from jax import lax
from jax.experimental import pallas as pl
from jax.experimental.pallas import tpu as pltpu
from jax.sharding import PartitionSpec as P

HEADS = 6
THIRDS = (0, 4, 8, 12)
CUTS = ((THIRDS, THIRDS), (THIRDS, (0, 4, 8, 10, 11, 12)))
COUNTS = [len(CUTS[n // 2][n % 2]) - 1 for n in range(4)]
PIECES = (3, 5)

epsilon = 1e-06
score_scale = 0.12
MESH = pl.DeviceIdType.MESH


def norm_rows(tensor):
    return tensor * lax.rsqrt(jnp.mean(tensor * tensor, axis=-1, keepdims=True) + epsilon)


def project(normed, weight):
    return jnp.dot(normed, weight, preferred_element_type=jnp.float32)


def kernel(
    sections,
    inputs_ref,
    wq_hbm,
    wk_hbm,
    wv_hbm,
    wo_hbm,
    mixing_ref,
    out_ref,
    wq,
    wk,
    wv,
    wo,
    h_in,
    h_out,
    v_buf,
    q_buf,
    k_buf,
    val_buf,
    p_buf,
    att_buf,
    acc_buf,
    in_sem,
    wv_sem,
    load_sem,
    hs_sem,
    hr_sem,
    vs_sem,
    vr_sem,
    os_sem,
    or_sem,
):
    me = lax.axis_index("section")
    last = sections - 1
    micro, rows, width = h_in.shape
    features = v_buf.shape[2]
    head = features // HEADS
    chunks = HEADS // 2
    span = features // chunks
    share = micro // sections
    is_first = me == 0
    is_last = me == last
    bf16 = jnp.bfloat16
    f32 = jnp.float32

    def head_part(n):
        return slice(n * head, (n + 1) * head)

    def chunk_part(j):
        return slice(j * span, (j + 1) * span)

    def input_load(i):
        return pltpu.make_async_copy(inputs_ref.at[i], h_in.at[i], in_sem.at[i])

    def value_load(j):
        return pltpu.make_async_copy(
            wv_hbm.at[0, :, chunk_part(j)], wv.at[:, chunk_part(j)], wv_sem.at[j]
        )

    loads = [
        pltpu.make_async_copy(source.at[0], target, load_sem.at[i])
        for i, (source, target) in enumerate(((wq_hbm, wq), (wk_hbm, wk), (wo_hbm, wo)))
    ]

    barrier = pltpu.get_barrier_semaphore()
    for step in range(1, sections):
        pl.semaphore_signal(
            barrier,
            inc=1,
            device_id={"section": lax.rem(me + step, sections)},
            device_id_type=MESH,
        )

    @pl.when(is_first)
    def _():
        input_load(0).start()

    for j in range(chunks):
        value_load(j).start()
    for load in loads:
        load.start()

    @pl.when(is_first)
    def _():
        for i in range(1, micro):
            input_load(i).start()

    pl.semaphore_wait(barrier, sections - 1)

    onward = jnp.minimum(me + 1, last)

    def h_copy(i):
        return pltpu.make_async_remote_copy(
            src_ref=h_out.at[i],
            dst_ref=h_in.at[i],
            send_sem=hs_sem.at[i],
            recv_sem=hr_sem.at[i],
            device_id={"section": onward},
            device_id_type=MESH,
        )

    def v_copy(i, j):
        return pltpu.make_async_remote_copy(
            src_ref=v_buf.at[i, :, chunk_part(j)],
            dst_ref=v_buf.at[i, :, chunk_part(j)],
            send_sem=vs_sem.at[i, j],
            recv_sem=vr_sem.at[i, j],
            device_id={"section": onward},
            device_id_type=MESH,
        )

    def out_copy(i):
        return pltpu.make_async_remote_copy(
            src_ref=h_out.at[i],
            dst_ref=out_ref.at[i % share],
            send_sem=os_sem.at[i],
            recv_sem=or_sem.at[i],
            device_id={"section": i // share},
            device_id_type=MESH,
        )

    row_index = lax.broadcasted_iota(jnp.int32, (rows, rows), 0)
    column_index = lax.broadcasted_iota(jnp.int32, (rows, rows), 1)
    causal = row_index >= column_index

    def fill_probabilities(normed):
        queries = project(normed, wq[...])
        key_rows = project(normed, wk[...])
        for n in range(HEADS):
            q_buf[:, head_part(n)] = norm_rows(queries[:, head_part(n)]).astype(bf16)
            k_buf[:, head_part(n)] = norm_rows(key_rows[:, head_part(n)]).astype(bf16)
        for n in range(HEADS):
            scores = (
                lax.dot_general(
                    q_buf[:, head_part(n)],
                    k_buf[:, head_part(n)],
                    (((1,), (1,)), ((), ())),
                    preferred_element_type=f32,
                )
                * score_scale
            )
            weights = jnp.where(causal, jnp.exp(scores), 0.0)
            p_buf[n] = (weights / jnp.sum(weights, axis=-1, keepdims=True)).astype(bf16)

    @pl.when(is_first)
    def _():
        def one(i, carry):
            input_load(i).wait()
            normed = norm_rows(h_in[i].astype(f32)).astype(bf16)
            for j in range(chunks):

                @pl.when(i == 0)
                def _():
                    value_load(j).wait()

                v_buf[i, :, chunk_part(j)] = project(normed, wv[:, chunk_part(j)]).astype(bf16)
                if sections > 1:

                    @pl.when(i == 0)
                    def _():
                        v_copy(i, j).start()

            @pl.when(i == 0)
            def _():
                for load in loads:
                    load.wait()

            fill_probabilities(normed)
            for n in range(HEADS):
                att_buf[:, head_part(n)] = project(p_buf[n], v_buf[i, :, head_part(n)]).astype(bf16)
            result = (h_in[i].astype(f32) + project(att_buf[...], wo[...])).astype(bf16)
            if sections > 1:
                h_out[i] = result
                h_copy(i).start()

                @pl.when(i > 0)
                def _():
                    for j in range(chunks):
                        v_copy(i, j).start()

            else:
                out_ref[i] = result
            return carry

        lax.fori_loop(0, micro, one, 0)

    if sections > 1:

        @pl.when(jnp.logical_not(is_first))
        def _():
            for j in range(chunks):
                value_load(j).wait()
            for load in loads:
                load.wait()
            mixing = mixing_ref[0]

            def one(i, carry):
                h_copy(i).wait_recv()
                normed = norm_rows(h_in[i].astype(f32)).astype(bf16)
                fill_probabilities(normed)
                val_buf[...] = mixing * project(normed, wv[...])
                for j in range(chunks):
                    v_copy(i, j).wait_recv()
                    if sections > 2:

                        @pl.when(jnp.logical_not(is_last))
                        def _():
                            v_copy(i, j).start()

                    used = (
                        val_buf[:, chunk_part(j)]
                        + (1.0 - mixing) * v_buf[i, :, chunk_part(j)].astype(f32)
                    ).astype(bf16)
                    for n in range(2):
                        att_buf[:, head_part(2 * j + n)] = project(
                            p_buf[2 * j + n], used[:, head_part(n)]
                        ).astype(bf16)
                    term = project(att_buf[:, chunk_part(j)], wo[chunk_part(j), :])
                    if j == 0:
                        acc_buf[...] = term
                    elif j < chunks - 1:
                        acc_buf[...] += term
                result = (h_in[i].astype(f32) + (acc_buf[...] + term)).astype(bf16)
                mine = jnp.logical_and(is_last, i // share == last)

                @pl.when(mine)
                def _():
                    out_ref[i % share] = result

                @pl.when(jnp.logical_not(mine))
                def _():
                    h_out[i] = result

                    @pl.when(is_last)
                    def _():
                        out_copy(i).start()

                    if sections > 2:

                        @pl.when(jnp.logical_not(is_last))
                        def _():
                            h_copy(i).start()

                return carry

            lax.fori_loop(0, micro, one, 0)

    @pl.when(jnp.logical_not(is_last))
    def _():
        for i in range(micro):
            for j in range(chunks):
                v_copy(i, j).wait_send()
            h_copy(i).wait_send()

    for i in range(micro):
        if i // share != last:

            @pl.when(is_last)
            def _():
                out_copy(i).wait_send()

            @pl.when(me == i // share)
            def _():
                out_copy(i).wait_recv()


def body(inputs, w_query, w_key, w_value, w_out, mixing):
    sections = lax.axis_size("section")
    micro, rows, width = inputs.shape
    features = w_value.shape[2]
    share = micro // sections
    bf16 = jnp.bfloat16
    anywhere = pl.BlockSpec(memory_space=pltpu.HBM)
    dma = pltpu.SemaphoreType.DMA
    return pl.pallas_call(
        functools.partial(kernel, sections),
        out_shape=pltpu.VMEM((share, rows, width), bf16),
        in_specs=[anywhere] * 5 + [pl.BlockSpec(memory_space=pltpu.SMEM)],
        out_specs=pl.BlockSpec(memory_space=pltpu.VMEM),
        scratch_shapes=[
            pltpu.VMEM((width, features), bf16),
            pltpu.VMEM((width, features), bf16),
            pltpu.VMEM((width, features), bf16),
            pltpu.VMEM((features, width), bf16),
            pltpu.VMEM((micro, rows, width), bf16),
            pltpu.VMEM((micro, rows, width), bf16),
            pltpu.VMEM((micro, rows, features), bf16),
            pltpu.VMEM((rows, features), bf16),
            pltpu.VMEM((rows, features), bf16),
            pltpu.VMEM((rows, features), jnp.float32),
            pltpu.VMEM((HEADS, rows, rows), bf16),
            pltpu.VMEM((rows, features), bf16),
            pltpu.VMEM((rows, width), jnp.float32),
            dma((micro,)),
            dma((HEADS // 2,)),
            dma((3,)),
            dma((micro,)),
            dma((micro,)),
            dma((micro, HEADS // 2)),
            dma((micro, HEADS // 2)),
            dma((micro,)),
            dma((micro,)),
        ],
        compiler_params=pltpu.CompilerParams(
            collective_id=0, has_side_effects=True, vmem_limit_bytes=62 * 1024 * 1024
        ),
        name="sections",
    )(inputs, w_query, w_key, w_value, w_out, mixing)


def pair_kernel(
    inputs_ref,
    wq_hbm,
    wk_hbm,
    wv_hbm,
    wo_hbm,
    mixing_ref,
    out_ref,
    wq,
    wk,
    wv,
    wo,
    wx,
    h_in,
    h_out,
    normed_buf,
    v_buf,
    q_buf,
    k_buf,
    used_buf,
    p_buf,
    low_buf,
    high_buf,
    att_buf,
    q_acc,
    k_acc,
    v_acc,
    val_buf,
    out_acc,
    load_sem,
    send_sem,
    recv_sem,
    met_sem,
):
    me = lax.axis_index("section")
    dp = lax.axis_index("dp")
    core = dp % 2
    across = dp + 2 - 4 * ((dp // 2) % 2)
    along = dp + 4 - 8 * ((dp // 4) % 2)
    beside = dp + 1 - 2 * core
    near = (dp // 2 + dp // 4) % 2
    most = max(PIECES)
    column = dp // 2 % 2
    mine, missed = most - 1 - column, most - 2 + column
    micro, rows, width = h_in.shape
    features = wv.shape[1]
    head = features // HEADS
    chunks = HEADS // 2
    span = features // chunks
    half = rows // 2
    share = features // 2
    piece = share // sum(PIECES)
    bf16 = jnp.bfloat16
    f32 = jnp.float32
    everything = slice(0, rows)
    early = slice(0, (chunks - 1) * span)
    late = slice((chunks - 1) * span, features)

    def head_part(n):
        return slice(n * head, (n + 1) * head)

    def chunk_part(j):
        return slice(j * span, (j + 1) * span)

    def cut_parts(i, t):
        ends = [width * n // 12 for n in CUTS[i][t]]
        return [slice(*pair) for pair in zip(ends, ends[1:])]

    def half_part(t):
        return slice(t * half, (t + 1) * half)

    def sequence_part(i):
        return slice(i * rows, (i + 1) * rows)

    def load(source, target, n):
        return pltpu.make_async_copy(source, target, load_sem.at[n])

    def input_load(i):
        return load(inputs_ref.at[i], h_in.at[i], i)

    def value_load(j):
        return load(wv_hbm.at[0, :, chunk_part(j)], wv.at[:, chunk_part(j)], 2 + j)

    query_load = load(wq_hbm.at[0], wq, 5)
    key_load = load(wk_hbm.at[0], wk, 6)
    out_load = load(wo_hbm.at[0], wo, 7)
    values_load = load(wv_hbm.at[0], wv, 2)

    def share_load(r):
        part = pl.ds(pl.multiple_of((near + r) % 2 * share, share), share)
        return load(wo_hbm.at[0, part, :], wo.at[part, :], r)

    def send(source, target, sent, received, device):
        return pltpu.make_async_remote_copy(
            src_ref=source,
            dst_ref=target,
            send_sem=send_sem.at[sent],
            recv_sem=recv_sem.at[received],
            device_id=device,
            device_id_type=MESH,
        )

    def cut_copy(i, t, c):
        part = (i, half_part(t), cut_parts(i, t)[c])
        place = sum(COUNTS[: 2 * i + t]) + c
        return send(h_out.at[part], h_in.at[part], 0 if i or t else 4, place, {"section": 1})

    def v_copy(part, n):
        return send(v_buf.at[1, :, part], v_buf.at[1, :, part], 1, sum(COUNTS) + n, {"section": 1})

    def low_copy():
        return send(low_buf, low_buf, 2, 0, {"section": 0})

    def high_copy(g):
        return send(high_buf.at[g], high_buf.at[g], 3, 1 + g, {"section": 0})

    def piece_part(far, i):
        start = (near + far) % 2 * share + core * PIECES[0] * piece + i * piece
        return pl.ds(pl.multiple_of(start, piece), piece)

    def y_copy(i):
        part = piece_part(0, i)
        sent = 1 if i else core
        return send(wo.at[part, :], wx.at[part, :], sent, 3 + i, {"section": 0})

    def side_copy(far, i):
        part = wx.at[piece_part(far, i), :]
        return send(part, part, 2, 3 + most + i, {"dp": along if i % 2 else across})

    def rare_copy():
        part = piece_part(0, mine)
        return send(wo.at[part, :], wx.at[part, :], 0, 1 + most, {"section": 0})

    def rare_side(step):
        part = wx.at[piece_part(0, mine), :]
        return send(part, part, 2, 1 + 2 * most + step, {"dp": across if step else along})

    def relay_copy():
        part = wx.at[piece_part(1, missed), :]
        return send(part, part, 2, 2 + most, {"dp": along})

    def core_copy(far, i):
        part = wx.at[piece_part(far, i), :]
        return send(part, part, 3, 3 + 2 * most, {"dp": beside})

    def pieces_wait(count, sent, received):
        part = wx.at[: count * piece, :]
        return send(part, part, sent, received, {"dp": beside})

    def rows_sent(count, sent):
        part = wx.at[:count, :]
        return send(part, part, sent, 0, {"section": 1})

    def for_core(run):
        for n in range(2):
            pl.when(core == n)(functools.partial(run, PIECES[n], PIECES[1 - n]))

    barrier = pltpu.get_barrier_semaphore()

    @pl.when(me == 1)
    def _():
        share_load(0).start()
        pl.semaphore_wait(barrier, 1)
        pl.semaphore_signal(met_sem, inc=1, device_id={"section": 0}, device_id_type=MESH)

    @pl.when(me == 0)
    def _():
        for device in ({"section": 1}, {"dp": across}, {"dp": along}, {"dp": beside}):
            pl.semaphore_signal(barrier, inc=1, device_id=device, device_id_type=MESH)

    row_index = lax.broadcasted_iota(jnp.int32, (rows, rows), 0)
    column_index = lax.broadcasted_iota(jnp.int32, (rows, rows), 1)
    causal = row_index >= column_index

    def normed_rows(values):
        return norm_rows(values.astype(f32)).astype(bf16)

    def fill_heads(target, part, values):
        for n in range(HEADS):
            target[part, head_part(n)] = norm_rows(values[:, head_part(n)]).astype(bf16)

    def probabilities(part, keys, n):
        scores = (
            lax.dot_general(
                q_buf[part, head_part(n)],
                k_buf[:keys, head_part(n)],
                (((1,), (1,)), ((), ())),
                preferred_element_type=f32,
            )
            * score_scale
        )
        weights = jnp.where(causal[part, :keys], jnp.exp(scores), 0.0)
        return weights / jnp.sum(weights, axis=-1, keepdims=True)

    @pl.when(me == 0)
    def _():
        input_load(1).start()
        value_load(0).start()
        input_load(0).start()
        for j in range(1, chunks):
            value_load(j).start()

        def fill_normed(i):
            with jax.named_scope(f"in{i}"):
                input_load(i).wait()
            normed_buf[sequence_part(i), :] = normed_rows(h_in[i])

        def fill_values(i, j):
            v_buf[i, :, chunk_part(j)] = project(
                normed_buf[sequence_part(i), :], wv[:, chunk_part(j)]
            ).astype(bf16)

        fill_normed(1)
        query_load.start()
        key_load.start()
        out_load.start()
        for j in range(chunks - 1):
            with jax.named_scope(f"wv{j}"):
                value_load(j).wait()
            fill_values(1, j)
            if j == 0:
                with jax.named_scope("met"):
                    pl.semaphore_wait(met_sem, 1)
            v_copy(chunk_part(j), 0).start()
        value_load(chunks - 1).wait()

        @pl.when(core == 0)
        def _():
            fill_values(1, chunks - 1)
            v_copy(late, 1).start()

        fill_normed(0)
        for j in range(chunks):
            fill_values(0, j)

        def fill_queries(i):
            normed = normed_buf[sequence_part(i), :]
            if i == 0:
                with jax.named_scope("wq"):
                    query_load.wait()
            fill_heads(q_buf, everything, project(normed, wq[...]))
            if i == 0:
                with jax.named_scope("wk"):
                    key_load.wait()
            fill_heads(k_buf, everything, project(normed, wk[...]))

        def attend(i, part, keys):
            for n in range(HEADS):
                p_buf[n, part, :keys] = probabilities(part, keys, n).astype(bf16)
            for n in range(HEADS):
                att_buf[part, head_part(n)] = project(
                    p_buf[n, part, :keys], v_buf[i, :keys, head_part(n)]
                ).astype(bf16)

        def next_rows(i, t):
            part = half_part(t)
            for c, columns in enumerate(cut_parts(i, t)):
                h_out[i, part, columns] = (
                    h_in[i, part, columns].astype(f32) + project(att_buf[part, :], wo[:, columns])
                ).astype(bf16)
                if (i, t) == (0, 0):
                    cut_copy(i, t, c).start()

        def start_rows(i, t):
            for c in range(COUNTS[2 * i + t]):
                cut_copy(i, t, c).start()

        def pass_on(i):
            with jax.named_scope(f"pass{i}"):
                y_copy(i).wait_recv()
            side_copy(0, i).start()
            core_copy(0, i).start()

        def pass_far(i):
            with jax.named_scope(f"far{i}"):
                side_copy(1, i).wait_recv()
            core_copy(1, i).start()

        fill_queries(0)
        for t in range(2):
            attend(0, half_part(t), (t + 1) * half)
            if t == 0:
                with jax.named_scope("wo"):
                    out_load.wait()
            with jax.named_scope(f"h0{t}"):
                next_rows(0, t)
        pl.when(core == 0)(functools.partial(start_rows, 0, 1))
        pl.when(core == 1)(functools.partial(fill_values, 1, chunks - 1))
        with jax.named_scope("bar"):
            pl.semaphore_wait(barrier, 3)

        @pl.when(core == 1)
        def _():
            with jax.named_scope("rare"):
                rare_copy().wait_recv()
            for step in range(2):
                rare_side(step).start()
            core_copy(0, mine).start()

        pl.when(core == 0)(functools.partial(pass_on, 0))
        fill_queries(1)
        attend(1, everything, rows)
        with jax.named_scope("h1"):
            for t in range(2):
                next_rows(1, t)
                pl.when(core == 0)(functools.partial(start_rows, 1, t))

        @pl.when(core == 1)
        def _():
            with jax.named_scope("yield"):
                rows_sent(half, 4).wait_send()
            start_rows(0, 1)
            for t in range(2):
                start_rows(1, t)

        pl.when(core == 1)(lambda: v_copy(late, 1).start())
        pl.when(core == 1)(functools.partial(pass_on, 0))
        pass_on(1)

        @pl.when(core == 1)
        def _():
            with jax.named_scope("across"):
                rare_side(1).wait_recv()
            relay_copy().start()
            core_copy(1, missed).start()
            with jax.named_scope("along"):
                rare_side(0).wait_recv()
            core_copy(1, mine).start()

        pass_far(0)
        for i in range(2, min(PIECES)):
            pass_on(i)
            pass_far(i - 1)

        @pl.when(core == 1)
        def _():
            with jax.named_scope("relay"):
                relay_copy().wait_recv()
            core_copy(0, missed).start()

        pass_far(min(PIECES) - 1)
        with jax.named_scope("core"):
            for_core(lambda own, other: pieces_wait(2 * other, 3, 3 + 2 * most).wait_recv())
        for t in range(2):
            part = half_part(t)
            keys = (t + 1) * half
            for n in range(HEADS):
                group, place = n // chunks, n % chunks
                if t == 0:
                    if n == 0:
                        with jax.named_scope("low"):
                            low_copy().wait_recv()
                    passed = low_buf[n // 2, :, n % 2 * half : (n % 2 + 1) * half]
                    own = low_buf[chunks + n]
                else:
                    if place == 0:
                        with jax.named_scope(f"high{group}"):
                            high_copy(group).wait_recv()
                    passed = high_buf[group, place]
                    own = high_buf[group, chunks + place]
                att_buf[part, head_part(n)] = (
                    own.astype(f32) + project(passed, v_buf[0, :keys, head_part(n)])
                ).astype(bf16)
            out_ref[0, part, :] = (
                h_out[0, part, :].astype(f32) + project(att_buf[part, :], wx[...])
            ).astype(bf16)
        with jax.named_scope("end"):
            pl.when(core == 0)(rows_sent(half, 4).wait_send)
            rows_sent(3 * half, 0).wait_send()
            send(v_buf.at[1], v_buf.at[1], 1, 0, {"section": 1}).wait_send()
            for_core(lambda own, other: pieces_wait(own + own // most, 2, 0).wait_send())
            for_core(lambda own, other: pieces_wait(2 * own, 3, 0).wait_send())

    @pl.when(me == 1)
    def _():
        mixing = mixing_ref[0]
        with jax.named_scope("wo"):
            share_load(0).wait()
        pl.when(core == 1)(lambda: rare_copy().start())
        for i in range(min(PIECES)):
            y_copy(i).start()
        with jax.named_scope("y0"):
            pieces_wait(1, 0, 0).wait_send()
        query_load.start()
        key_load.start()
        values_load.start()
        share_load(1).start()
        with jax.named_scope("loads"):
            query_load.wait()
            key_load.wait()
            values_load.wait()
            share_load(1).wait()

        def fill_rows(i, t):
            part = half_part(t)
            squares = jnp.zeros((half, 1), f32)
            for c, columns in enumerate(cut_parts(i, t)):
                with jax.named_scope(f"cut{i}{t}{c}"):
                    cut_copy(i, t, c).wait_recv()
                arrived = h_in[i, part, columns]
                for target, weight in ((q_acc, wq), (k_acc, wk), (v_acc, wv)):
                    term = project(arrived, weight[columns, :])
                    if c == 0:
                        target[...] = term
                    else:
                        target[...] += term
                wide = arrived.astype(f32)
                squares += jnp.sum(wide * wide, axis=-1, keepdims=True)
            scale = lax.rsqrt(squares / width + epsilon)
            fill_heads(q_buf, part, q_acc[...] * scale)
            fill_heads(k_buf, part, k_acc[...] * scale)
            return mixing * (v_acc[...] * scale)

        for t in range(2):
            part = half_part(t)
            keys = (t + 1) * half
            used_buf[part, :] = fill_rows(0, t).astype(bf16)
            for n in range(HEADS):
                group, place = n // chunks, n % chunks
                shares = probabilities(part, keys, n)
                passed = ((1.0 - mixing) * shares).astype(bf16)
                own = project(shares.astype(bf16), used_buf[:keys, head_part(n)]).astype(bf16)
                if t == 0:
                    low_buf[n // 2, :, n % 2 * half : (n % 2 + 1) * half] = passed
                    low_buf[chunks + n] = own
                else:
                    high_buf[group, place] = passed
                    high_buf[group, chunks + place] = own
                    if place == chunks - 1:
                        high_copy(group).start()
            if t == 0:
                low_copy().start()

        def fill_used(part, columns):
            used_buf[part, columns] = (
                val_buf[part, columns] + (1.0 - mixing) * v_buf[1, part, columns].astype(f32)
            ).astype(bf16)

        def fill_attended(t, heads):
            part = half_part(t)
            keys = (t + 1) * half
            for n in heads:
                att_buf[part, head_part(n)] = project(
                    p_buf[n, part, :keys], used_buf[:keys, head_part(n)]
                ).astype(bf16)

        def finish_rows(t, columns):
            part = half_part(t)
            keys = (t + 1) * half
            for n in range(HEADS):
                p_buf[n, part, :keys] = probabilities(part, keys, n).astype(bf16)
            fill_used(part, columns)
            fill_attended(t, range(columns.stop // head))
            return h_in[1, part, :].astype(f32) + project(att_buf[part, columns], wo[columns, :])

        def finish_either(t):
            @pl.when(core == 0)
            def _():
                if t == 0:
                    v_copy(late, 1).wait_recv()
                out_ref[0, half_part(t), :] = finish_rows(t, slice(0, features)).astype(bf16)

            @pl.when(core == 1)
            def _():
                out_acc[half_part(t), :] = finish_rows(t, early)

        val_buf[half_part(0), :] = fill_rows(1, 0)
        v_copy(early, 0).wait_recv()
        finish_either(0)
        val_buf[half_part(1), :] = fill_rows(1, 1)
        with jax.named_scope("last"):
            finish_either(1)

        @pl.when(core == 1)
        def _():
            with jax.named_scope("first"):
                v_copy(late, 1).wait_recv()
            with jax.named_scope("out"):
                fill_used(everything, late)
                for t in range(2):
                    fill_attended(t, range(HEADS - 2, HEADS))
                out_ref[0] = (out_acc[...] + project(att_buf[:, late], wo[late, :])).astype(bf16)

        with jax.named_scope("end"):
            for_core(lambda own, other: pieces_wait(own - 1 - own // most, 1, 0).wait_send())
            send(low_buf, low_buf, 2, 0, {"section": 0}).wait_send()
            send(high_buf, high_buf, 3, 0, {"section": 0}).wait_send()


def pair_body(inputs, w_query, w_key, w_value, w_out, mixing):
    micro, rows, width = inputs.shape
    features = w_value.shape[2]
    half = rows // 2
    chunks = HEADS // 2
    head = features // HEADS
    bf16 = jnp.bfloat16
    f32 = jnp.float32
    anywhere = pl.BlockSpec(memory_space=pltpu.HBM)
    dma = pltpu.SemaphoreType.DMA
    return pl.pallas_call(
        pair_kernel,
        out_shape=pltpu.VMEM((1, rows, width), bf16),
        in_specs=[anywhere] * 5 + [pl.BlockSpec(memory_space=pltpu.SMEM)],
        out_specs=pl.BlockSpec(memory_space=pltpu.VMEM),
        scratch_shapes=[
            pltpu.VMEM((width, features), bf16),
            pltpu.VMEM((width, features), bf16),
            pltpu.VMEM((width, features), bf16),
            pltpu.VMEM((features, width), bf16),
            pltpu.VMEM((features, width), bf16),
            pltpu.VMEM((micro, rows, width), bf16),
            pltpu.VMEM((micro, rows, width), bf16),
            pltpu.VMEM((micro * rows, width), bf16),
            pltpu.VMEM((micro, rows, features), bf16),
            pltpu.VMEM((rows, features), bf16),
            pltpu.VMEM((rows, features), bf16),
            pltpu.VMEM((rows, features), bf16),
            pltpu.VMEM((HEADS, rows, rows), bf16),
            pltpu.VMEM((chunks + HEADS, half, head), bf16),
            pltpu.VMEM((2, HEADS, half, head), bf16),
            pltpu.VMEM((rows, features), bf16),
            pltpu.VMEM((half, features), f32),
            pltpu.VMEM((half, features), f32),
            pltpu.VMEM((half, features), f32),
            pltpu.VMEM((rows, features), f32),
            pltpu.VMEM((rows, width), f32),
            dma((8,)),
            dma((5,)),
            dma((max(2 + sum(COUNTS), 4 + 2 * max(PIECES)),)),
            pltpu.SemaphoreType.REGULAR,
        ],
        compiler_params=pltpu.CompilerParams(
            collective_id=0, has_side_effects=True, vmem_limit_bytes=62 * 1024 * 1024
        ),
        name="section_pair",
    )(inputs, w_query, w_key, w_value, w_out, mixing)


def solution(mesh):
    in_specs = (
        P("dp", None, None),
        P("section", None, None),
        P("section", None, None),
        P("section", None, None),
        P("section", None, None),
        P("section"),
    )
    out_specs = P(("dp", "section"), None, None)
    paired = mesh.shape["section"] == 2 and mesh.shape["dp"] % 8 == 0

    def either(inputs, *weights):
        square = inputs.shape[1] * HEADS == weights[2].shape[2]
        chosen = pair_body if paired and square and inputs.shape[0] == 2 else body
        return chosen(inputs, *weights)

    return jax.shard_map(either, mesh=mesh, in_specs=in_specs, out_specs=out_specs, check_vma=False)
```

```python
import functools

import jax
import jax.numpy as jnp
from jax import lax
from jax.experimental import pallas as pl
from jax.experimental.pallas import tpu as pltpu
from jax.sharding import PartitionSpec as P

HEADS = 6
THIRDS = (0, 4, 8, 12)
HALVES = (0, 6, 12)
CUTS = ((THIRDS, HALVES), (HALVES, (0, 4, 8, 10, 11, 12)))
COUNTS = [len(CUTS[n // 2][n % 2]) - 1 for n in range(4)]
PIECES = (3, 5)

epsilon = 1e-06
score_scale = 0.12
MESH = pl.DeviceIdType.MESH


def norm_rows(tensor):
    return tensor * lax.rsqrt(jnp.mean(tensor * tensor, axis=-1, keepdims=True) + epsilon)


def project(normed, weight):
    return jnp.dot(normed, weight, preferred_element_type=jnp.float32)


def kernel(
    sections,
    inputs_ref,
    wq_hbm,
    wk_hbm,
    wv_hbm,
    wo_hbm,
    mixing_ref,
    out_ref,
    wq,
    wk,
    wv,
    wo,
    h_in,
    h_out,
    v_buf,
    q_buf,
    k_buf,
    val_buf,
    p_buf,
    att_buf,
    acc_buf,
    in_sem,
    wv_sem,
    load_sem,
    hs_sem,
    hr_sem,
    vs_sem,
    vr_sem,
    os_sem,
    or_sem,
):
    me = lax.axis_index("section")
    last = sections - 1
    micro, rows, width = h_in.shape
    features = v_buf.shape[2]
    head = features // HEADS
    chunks = HEADS // 2
    span = features // chunks
    share = micro // sections
    is_first = me == 0
    is_last = me == last
    bf16 = jnp.bfloat16
    f32 = jnp.float32

    def head_part(n):
        return slice(n * head, (n + 1) * head)

    def chunk_part(j):
        return slice(j * span, (j + 1) * span)

    def input_load(i):
        return pltpu.make_async_copy(inputs_ref.at[i], h_in.at[i], in_sem.at[i])

    def value_load(j):
        return pltpu.make_async_copy(
            wv_hbm.at[0, :, chunk_part(j)], wv.at[:, chunk_part(j)], wv_sem.at[j]
        )

    loads = [
        pltpu.make_async_copy(source.at[0], target, load_sem.at[i])
        for i, (source, target) in enumerate(((wq_hbm, wq), (wk_hbm, wk), (wo_hbm, wo)))
    ]

    barrier = pltpu.get_barrier_semaphore()
    for step in range(1, sections):
        pl.semaphore_signal(
            barrier,
            inc=1,
            device_id={"section": lax.rem(me + step, sections)},
            device_id_type=MESH,
        )

    @pl.when(is_first)
    def _():
        input_load(0).start()

    for j in range(chunks):
        value_load(j).start()
    for load in loads:
        load.start()

    @pl.when(is_first)
    def _():
        for i in range(1, micro):
            input_load(i).start()

    pl.semaphore_wait(barrier, sections - 1)

    onward = jnp.minimum(me + 1, last)

    def h_copy(i):
        return pltpu.make_async_remote_copy(
            src_ref=h_out.at[i],
            dst_ref=h_in.at[i],
            send_sem=hs_sem.at[i],
            recv_sem=hr_sem.at[i],
            device_id={"section": onward},
            device_id_type=MESH,
        )

    def v_copy(i, j):
        return pltpu.make_async_remote_copy(
            src_ref=v_buf.at[i, :, chunk_part(j)],
            dst_ref=v_buf.at[i, :, chunk_part(j)],
            send_sem=vs_sem.at[i, j],
            recv_sem=vr_sem.at[i, j],
            device_id={"section": onward},
            device_id_type=MESH,
        )

    def out_copy(i):
        return pltpu.make_async_remote_copy(
            src_ref=h_out.at[i],
            dst_ref=out_ref.at[i % share],
            send_sem=os_sem.at[i],
            recv_sem=or_sem.at[i],
            device_id={"section": i // share},
            device_id_type=MESH,
        )

    row_index = lax.broadcasted_iota(jnp.int32, (rows, rows), 0)
    column_index = lax.broadcasted_iota(jnp.int32, (rows, rows), 1)
    causal = row_index >= column_index

    def fill_probabilities(normed):
        queries = project(normed, wq[...])
        key_rows = project(normed, wk[...])
        for n in range(HEADS):
            q_buf[:, head_part(n)] = norm_rows(queries[:, head_part(n)]).astype(bf16)
            k_buf[:, head_part(n)] = norm_rows(key_rows[:, head_part(n)]).astype(bf16)
        for n in range(HEADS):
            scores = (
                lax.dot_general(
                    q_buf[:, head_part(n)],
                    k_buf[:, head_part(n)],
                    (((1,), (1,)), ((), ())),
                    preferred_element_type=f32,
                )
                * score_scale
            )
            weights = jnp.where(causal, jnp.exp(scores), 0.0)
            p_buf[n] = (weights / jnp.sum(weights, axis=-1, keepdims=True)).astype(bf16)

    @pl.when(is_first)
    def _():
        def one(i, carry):
            input_load(i).wait()
            normed = norm_rows(h_in[i].astype(f32)).astype(bf16)
            for j in range(chunks):

                @pl.when(i == 0)
                def _():
                    value_load(j).wait()

                v_buf[i, :, chunk_part(j)] = project(normed, wv[:, chunk_part(j)]).astype(bf16)
                if sections > 1:

                    @pl.when(i == 0)
                    def _():
                        v_copy(i, j).start()

            @pl.when(i == 0)
            def _():
                for load in loads:
                    load.wait()

            fill_probabilities(normed)
            for n in range(HEADS):
                att_buf[:, head_part(n)] = project(p_buf[n], v_buf[i, :, head_part(n)]).astype(bf16)
            result = (h_in[i].astype(f32) + project(att_buf[...], wo[...])).astype(bf16)
            if sections > 1:
                h_out[i] = result
                h_copy(i).start()

                @pl.when(i > 0)
                def _():
                    for j in range(chunks):
                        v_copy(i, j).start()

            else:
                out_ref[i] = result
            return carry

        lax.fori_loop(0, micro, one, 0)

    if sections > 1:

        @pl.when(jnp.logical_not(is_first))
        def _():
            for j in range(chunks):
                value_load(j).wait()
            for load in loads:
                load.wait()
            mixing = mixing_ref[0]

            def one(i, carry):
                h_copy(i).wait_recv()
                normed = norm_rows(h_in[i].astype(f32)).astype(bf16)
                fill_probabilities(normed)
                val_buf[...] = mixing * project(normed, wv[...])
                for j in range(chunks):
                    v_copy(i, j).wait_recv()
                    if sections > 2:

                        @pl.when(jnp.logical_not(is_last))
                        def _():
                            v_copy(i, j).start()

                    used = (
                        val_buf[:, chunk_part(j)]
                        + (1.0 - mixing) * v_buf[i, :, chunk_part(j)].astype(f32)
                    ).astype(bf16)
                    for n in range(2):
                        att_buf[:, head_part(2 * j + n)] = project(
                            p_buf[2 * j + n], used[:, head_part(n)]
                        ).astype(bf16)
                    term = project(att_buf[:, chunk_part(j)], wo[chunk_part(j), :])
                    if j == 0:
                        acc_buf[...] = term
                    elif j < chunks - 1:
                        acc_buf[...] += term
                result = (h_in[i].astype(f32) + (acc_buf[...] + term)).astype(bf16)
                mine = jnp.logical_and(is_last, i // share == last)

                @pl.when(mine)
                def _():
                    out_ref[i % share] = result

                @pl.when(jnp.logical_not(mine))
                def _():
                    h_out[i] = result

                    @pl.when(is_last)
                    def _():
                        out_copy(i).start()

                    if sections > 2:

                        @pl.when(jnp.logical_not(is_last))
                        def _():
                            h_copy(i).start()

                return carry

            lax.fori_loop(0, micro, one, 0)

    @pl.when(jnp.logical_not(is_last))
    def _():
        for i in range(micro):
            for j in range(chunks):
                v_copy(i, j).wait_send()
            h_copy(i).wait_send()

    for i in range(micro):
        if i // share != last:

            @pl.when(is_last)
            def _():
                out_copy(i).wait_send()

            @pl.when(me == i // share)
            def _():
                out_copy(i).wait_recv()


def body(inputs, w_query, w_key, w_value, w_out, mixing):
    sections = lax.axis_size("section")
    micro, rows, width = inputs.shape
    features = w_value.shape[2]
    share = micro // sections
    bf16 = jnp.bfloat16
    anywhere = pl.BlockSpec(memory_space=pltpu.HBM)
    dma = pltpu.SemaphoreType.DMA
    return pl.pallas_call(
        functools.partial(kernel, sections),
        out_shape=pltpu.VMEM((share, rows, width), bf16),
        in_specs=[anywhere] * 5 + [pl.BlockSpec(memory_space=pltpu.SMEM)],
        out_specs=pl.BlockSpec(memory_space=pltpu.VMEM),
        scratch_shapes=[
            pltpu.VMEM((width, features), bf16),
            pltpu.VMEM((width, features), bf16),
            pltpu.VMEM((width, features), bf16),
            pltpu.VMEM((features, width), bf16),
            pltpu.VMEM((micro, rows, width), bf16),
            pltpu.VMEM((micro, rows, width), bf16),
            pltpu.VMEM((micro, rows, features), bf16),
            pltpu.VMEM((rows, features), bf16),
            pltpu.VMEM((rows, features), bf16),
            pltpu.VMEM((rows, features), jnp.float32),
            pltpu.VMEM((HEADS, rows, rows), bf16),
            pltpu.VMEM((rows, features), bf16),
            pltpu.VMEM((rows, width), jnp.float32),
            dma((micro,)),
            dma((HEADS // 2,)),
            dma((3,)),
            dma((micro,)),
            dma((micro,)),
            dma((micro, HEADS // 2)),
            dma((micro, HEADS // 2)),
            dma((micro,)),
            dma((micro,)),
        ],
        compiler_params=pltpu.CompilerParams(
            collective_id=0, has_side_effects=True, vmem_limit_bytes=62 * 1024 * 1024
        ),
        name="sections",
    )(inputs, w_query, w_key, w_value, w_out, mixing)


def pair_kernel(
    inputs_ref,
    wq_hbm,
    wk_hbm,
    wv_hbm,
    wo_hbm,
    mixing_ref,
    out_ref,
    wq,
    wk,
    wv,
    wo,
    wx,
    h_in,
    h_out,
    normed_buf,
    v_buf,
    q_buf,
    k_buf,
    used_buf,
    p_buf,
    low_buf,
    high_buf,
    att_buf,
    q_acc,
    k_acc,
    v_acc,
    val_buf,
    out_acc,
    load_sem,
    send_sem,
    recv_sem,
    met_sem,
):
    me = lax.axis_index("section")
    dp = lax.axis_index("dp")
    core = dp % 2
    across = dp + 2 - 4 * ((dp // 2) % 2)
    along = dp + 4 - 8 * ((dp // 4) % 2)
    beside = dp + 1 - 2 * core
    near = (dp // 2 + dp // 4) % 2
    most = max(PIECES)
    column = dp // 2 % 2
    mine, missed = most - 1 - column, most - 2 + column
    micro, rows, width = h_in.shape
    features = wv.shape[1]
    head = features // HEADS
    chunks = HEADS // 2
    span = features // chunks
    half = rows // 2
    share = features // 2
    piece = share // sum(PIECES)
    bf16 = jnp.bfloat16
    f32 = jnp.float32
    everything = slice(0, rows)
    early = slice(0, (chunks - 1) * span)
    late = slice((chunks - 1) * span, features)

    def head_part(n):
        return slice(n * head, (n + 1) * head)

    def chunk_part(j):
        return slice(j * span, (j + 1) * span)

    def cut_parts(i, t):
        ends = [width * n // 12 for n in CUTS[i][t]]
        return [slice(*pair) for pair in zip(ends, ends[1:])]

    def half_part(t):
        return slice(t * half, (t + 1) * half)

    def sequence_part(i):
        return slice(i * rows, (i + 1) * rows)

    def load(source, target, n):
        return pltpu.make_async_copy(source, target, n)

    def input_load(i):
        return load(inputs_ref.at[i], h_in.at[i], send_sem.at[i])

    def value_load(j):
        return load(wv_hbm.at[0, :, chunk_part(j)], wv.at[:, chunk_part(j)], load_sem.at[j])

    query_load = load(wq_hbm.at[0], wq, send_sem.at[2])
    key_load = load(wk_hbm.at[0], wk, send_sem.at[3])
    out_load = load(wo_hbm.at[0], wo, send_sem.at[4])
    values_load = load(wv_hbm.at[0], wv, load_sem.at[2])

    def share_load(r):
        part = pl.ds(pl.multiple_of((near + r) % 2 * share, share), share)
        return load(wo_hbm.at[0, part, :], wo.at[part, :], load_sem.at[r])

    def send(source, target, sent, received, device):
        return pltpu.make_async_remote_copy(
            src_ref=source,
            dst_ref=target,
            send_sem=send_sem.at[sent],
            recv_sem=recv_sem.at[received],
            device_id=device,
            device_id_type=MESH,
        )

    def cut_copy(i, t, c):
        part = (i, half_part(t), cut_parts(i, t)[c])
        place = sum(COUNTS[: 2 * i + t]) + c
        return send(h_out.at[part], h_in.at[part], 0 if i or t else 4, place, {"section": 1})

    def v_copy(part, n):
        return send(v_buf.at[1, :, part], v_buf.at[1, :, part], 1, sum(COUNTS) + n, {"section": 1})

    def low_copy():
        return send(low_buf, low_buf, 2, 0, {"section": 0})

    def high_copy(g):
        return send(high_buf.at[g], high_buf.at[g], 3, 1 + g, {"section": 0})

    def piece_part(far, i):
        start = (near + far) % 2 * share + core * PIECES[0] * piece + i * piece
        return pl.ds(pl.multiple_of(start, piece), piece)

    def y_copy(i):
        part = piece_part(0, i)
        sent = 1 if i else core
        return send(wo.at[part, :], wx.at[part, :], sent, 3 + i, {"section": 0})

    def side_copy(far, i):
        part = wx.at[piece_part(far, i), :]
        return send(part, part, 2, 3 + most + i, {"dp": along if i % 2 else across})

    def rare_copy():
        part = piece_part(0, mine)
        return send(wo.at[part, :], wx.at[part, :], 0, 1 + most, {"section": 0})

    def rare_side(step):
        part = wx.at[piece_part(0, mine), :]
        return send(part, part, 2, 1 + 2 * most + step, {"dp": across if step else along})

    def relay_copy():
        part = wx.at[piece_part(1, missed), :]
        return send(part, part, 2, 2 + most, {"dp": along})

    def core_copy(far, i):
        part = wx.at[piece_part(far, i), :]
        return send(part, part, 3, 3 + 2 * most, {"dp": beside})

    def pieces_wait(count, sent, received):
        part = wx.at[: count * piece, :]
        return send(part, part, sent, received, {"dp": beside})

    def rows_sent(count, sent):
        part = wx.at[:count, :]
        return send(part, part, sent, 0, {"section": 1})

    def for_core(run):
        for n in range(2):
            pl.when(core == n)(functools.partial(run, PIECES[n], PIECES[1 - n]))

    barrier = pltpu.get_barrier_semaphore()

    @pl.when(me == 1)
    def _():
        share_load(0).start()
        pl.semaphore_wait(barrier, 1)
        pl.semaphore_signal(met_sem, inc=1, device_id={"section": 0}, device_id_type=MESH)

    @pl.when(me == 0)
    def _():
        for device in ({"section": 1}, {"dp": across}, {"dp": along}, {"dp": beside}):
            pl.semaphore_signal(barrier, inc=1, device_id=device, device_id_type=MESH)

    row_index = lax.broadcasted_iota(jnp.int32, (rows, rows), 0)
    column_index = lax.broadcasted_iota(jnp.int32, (rows, rows), 1)
    causal = row_index >= column_index

    def normed_rows(values):
        return norm_rows(values.astype(f32)).astype(bf16)

    def fill_heads(target, part, values):
        for n in range(HEADS):
            target[part, head_part(n)] = norm_rows(values[:, head_part(n)]).astype(bf16)

    def probabilities(part, keys, n):
        scores = (
            lax.dot_general(
                q_buf[part, head_part(n)],
                k_buf[:keys, head_part(n)],
                (((1,), (1,)), ((), ())),
                preferred_element_type=f32,
            )
            * score_scale
        )
        weights = jnp.where(causal[part, :keys], jnp.exp(scores), 0.0)
        return weights / jnp.sum(weights, axis=-1, keepdims=True)

    @pl.when(me == 0)
    def _():
        input_load(1).start()
        value_load(0).start()
        input_load(0).start()
        for j in range(1, chunks):
            value_load(j).start()

        def fill_normed(i):
            with jax.named_scope(f"in{i}"):
                input_load(i).wait()
            normed_buf[sequence_part(i), :] = normed_rows(h_in[i])

        def fill_values(i, j):
            v_buf[i, :, chunk_part(j)] = project(
                normed_buf[sequence_part(i), :], wv[:, chunk_part(j)]
            ).astype(bf16)

        fill_normed(1)
        query_load.start()
        key_load.start()
        out_load.start()
        for j in range(chunks - 1):
            with jax.named_scope(f"wv{j}"):
                value_load(j).wait()
            fill_values(1, j)
            if j == 0:
                with jax.named_scope("met"):
                    pl.semaphore_wait(met_sem, 1)
            v_copy(chunk_part(j), 0).start()
        value_load(chunks - 1).wait()

        @pl.when(core == 0)
        def _():
            fill_values(1, chunks - 1)
            v_copy(late, 1).start()

        fill_normed(0)
        for j in range(chunks):
            fill_values(0, j)

        def fill_queries(i):
            normed = normed_buf[sequence_part(i), :]
            if i == 0:
                with jax.named_scope("wq"):
                    query_load.wait()
            fill_heads(q_buf, everything, project(normed, wq[...]))
            if i == 0:
                with jax.named_scope("wk"):
                    key_load.wait()
            fill_heads(k_buf, everything, project(normed, wk[...]))

        def attend(i, part, keys):
            for n in range(HEADS):
                p_buf[n, part, :keys] = probabilities(part, keys, n).astype(bf16)
            for n in range(HEADS):
                att_buf[part, head_part(n)] = project(
                    p_buf[n, part, :keys], v_buf[i, :keys, head_part(n)]
                ).astype(bf16)

        def next_rows(i, t):
            part = half_part(t)
            for c, columns in enumerate(cut_parts(i, t)):
                h_out[i, part, columns] = (
                    h_in[i, part, columns].astype(f32) + project(att_buf[part, :], wo[:, columns])
                ).astype(bf16)
                if (i, t) == (0, 0):
                    cut_copy(i, t, c).start()

        def start_rows(i, t):
            for c in range(COUNTS[2 * i + t]):
                cut_copy(i, t, c).start()

        def pass_on(i):
            with jax.named_scope(f"pass{i}"):
                y_copy(i).wait_recv()
            side_copy(0, i).start()
            core_copy(0, i).start()

        def pass_far(i):
            with jax.named_scope(f"far{i}"):
                side_copy(1, i).wait_recv()
            core_copy(1, i).start()

        fill_queries(0)
        for t in range(2):
            attend(0, half_part(t), (t + 1) * half)
            if t == 0:
                with jax.named_scope("wo"):
                    out_load.wait()
            with jax.named_scope(f"h0{t}"):
                next_rows(0, t)
        pl.when(core == 0)(functools.partial(start_rows, 0, 1))
        pl.when(core == 1)(functools.partial(fill_values, 1, chunks - 1))
        with jax.named_scope("bar"):
            pl.semaphore_wait(barrier, 3)

        @pl.when(core == 1)
        def _():
            with jax.named_scope("rare"):
                rare_copy().wait_recv()
            for step in range(2):
                rare_side(step).start()
            core_copy(0, mine).start()

        pl.when(core == 0)(functools.partial(pass_on, 0))
        fill_queries(1)
        attend(1, everything, rows)
        with jax.named_scope("h1"):
            for t in range(2):
                next_rows(1, t)
                pl.when(core == 0)(functools.partial(start_rows, 1, t))

        @pl.when(core == 1)
        def _():
            with jax.named_scope("yield"):
                rows_sent(half, 4).wait_send()
            start_rows(0, 1)
            for t in range(2):
                start_rows(1, t)

        pl.when(core == 1)(lambda: v_copy(late, 1).start())
        pl.when(core == 1)(functools.partial(pass_on, 0))
        pass_on(1)

        @pl.when(core == 1)
        def _():
            with jax.named_scope("across"):
                rare_side(1).wait_recv()
            relay_copy().start()
            core_copy(1, missed).start()
            with jax.named_scope("along"):
                rare_side(0).wait_recv()
            core_copy(1, mine).start()

        pass_far(0)
        for i in range(2, min(PIECES)):
            pass_on(i)
            pass_far(i - 1)

        @pl.when(core == 1)
        def _():
            with jax.named_scope("relay"):
                relay_copy().wait_recv()
            core_copy(0, missed).start()

        pass_far(min(PIECES) - 1)
        with jax.named_scope("core"):
            for_core(lambda own, other: pieces_wait(2 * other, 3, 3 + 2 * most).wait_recv())
        for t in range(2):
            part = half_part(t)
            keys = (t + 1) * half
            for n in range(HEADS):
                group, place = n // chunks, n % chunks
                if t == 0:
                    if n == 0:
                        with jax.named_scope("low"):
                            low_copy().wait_recv()
                    passed = low_buf[n // 2, :, n % 2 * half : (n % 2 + 1) * half]
                    own = low_buf[chunks + n]
                else:
                    if place == 0:
                        with jax.named_scope(f"high{group}"):
                            high_copy(group).wait_recv()
                    passed = high_buf[group, place]
                    own = high_buf[group, chunks + place]
                att_buf[part, head_part(n)] = (
                    own.astype(f32) + project(passed, v_buf[0, :keys, head_part(n)])
                ).astype(bf16)
            out_ref[0, part, :] = (
                h_out[0, part, :].astype(f32) + project(att_buf[part, :], wx[...])
            ).astype(bf16)
        with jax.named_scope("end"):
            pl.when(core == 0)(rows_sent(half, 4).wait_send)
            rows_sent(3 * half, 0).wait_send()
            send(v_buf.at[1], v_buf.at[1], 1, 0, {"section": 1}).wait_send()
            for_core(lambda own, other: pieces_wait(own + own // most, 2, 0).wait_send())
            for_core(lambda own, other: pieces_wait(2 * own, 3, 0).wait_send())

    @pl.when(me == 1)
    def _():
        mixing = mixing_ref[0]
        with jax.named_scope("wo"):
            share_load(0).wait()
        pl.when(core == 1)(lambda: rare_copy().start())
        for i in range(min(PIECES)):
            y_copy(i).start()
        with jax.named_scope("y0"):
            pieces_wait(1, 0, 0).wait_send()
        query_load.start()
        key_load.start()
        values_load.start()
        share_load(1).start()
        with jax.named_scope("loads"):
            query_load.wait()
            key_load.wait()
            values_load.wait()
            share_load(1).wait()

        def fill_rows(i, t):
            part = half_part(t)
            squares = jnp.zeros((half, 1), f32)
            for c, columns in enumerate(cut_parts(i, t)):
                with jax.named_scope(f"cut{i}{t}{c}"):
                    cut_copy(i, t, c).wait_recv()
                arrived = h_in[i, part, columns]
                for target, weight in ((q_acc, wq), (k_acc, wk), (v_acc, wv)):
                    term = project(arrived, weight[columns, :])
                    if c == 0:
                        target[...] = term
                    else:
                        target[...] += term
                wide = arrived.astype(f32)
                squares += jnp.sum(wide * wide, axis=-1, keepdims=True)
            scale = lax.rsqrt(squares / width + epsilon)
            fill_heads(q_buf, part, q_acc[...] * scale)
            fill_heads(k_buf, part, k_acc[...] * scale)
            return mixing * (v_acc[...] * scale)

        for t in range(2):
            part = half_part(t)
            keys = (t + 1) * half
            used_buf[part, :] = fill_rows(0, t).astype(bf16)
            for n in range(HEADS):
                group, place = n // chunks, n % chunks
                shares = probabilities(part, keys, n)
                passed = ((1.0 - mixing) * shares).astype(bf16)
                own = project(shares.astype(bf16), used_buf[:keys, head_part(n)]).astype(bf16)
                if t == 0:
                    low_buf[n // 2, :, n % 2 * half : (n % 2 + 1) * half] = passed
                    low_buf[chunks + n] = own
                else:
                    high_buf[group, place] = passed
                    high_buf[group, chunks + place] = own
                    if place == chunks - 1:
                        high_copy(group).start()
            if t == 0:
                low_copy().start()

        def fill_used(part, columns):
            used_buf[part, columns] = (
                val_buf[part, columns] + (1.0 - mixing) * v_buf[1, part, columns].astype(f32)
            ).astype(bf16)

        def fill_attended(t, heads):
            part = half_part(t)
            keys = (t + 1) * half
            for n in heads:
                att_buf[part, head_part(n)] = project(
                    p_buf[n, part, :keys], used_buf[:keys, head_part(n)]
                ).astype(bf16)

        def finish_rows(t, columns):
            part = half_part(t)
            keys = (t + 1) * half
            for n in range(HEADS):
                p_buf[n, part, :keys] = probabilities(part, keys, n).astype(bf16)
            fill_used(part, columns)
            fill_attended(t, range(columns.stop // head))
            return h_in[1, part, :].astype(f32) + project(att_buf[part, columns], wo[columns, :])

        def finish_either(t):
            @pl.when(core == 0)
            def _():
                if t == 0:
                    v_copy(late, 1).wait_recv()
                out_ref[0, half_part(t), :] = finish_rows(t, slice(0, features)).astype(bf16)

            @pl.when(core == 1)
            def _():
                out_acc[half_part(t), :] = finish_rows(t, early)

        val_buf[half_part(0), :] = fill_rows(1, 0)
        v_copy(early, 0).wait_recv()
        finish_either(0)
        val_buf[half_part(1), :] = fill_rows(1, 1)
        with jax.named_scope("last"):
            finish_either(1)

        @pl.when(core == 1)
        def _():
            with jax.named_scope("first"):
                v_copy(late, 1).wait_recv()
            with jax.named_scope("out"):
                fill_used(everything, late)
                for t in range(2):
                    fill_attended(t, range(HEADS - 2, HEADS))
                out_ref[0] = (out_acc[...] + project(att_buf[:, late], wo[late, :])).astype(bf16)

        with jax.named_scope("end"):
            for_core(lambda own, other: pieces_wait(own - 1 - own // most, 1, 0).wait_send())
            send(low_buf, low_buf, 2, 0, {"section": 0}).wait_send()
            send(high_buf, high_buf, 3, 0, {"section": 0}).wait_send()


def pair_body(inputs, w_query, w_key, w_value, w_out, mixing):
    micro, rows, width = inputs.shape
    features = w_value.shape[2]
    half = rows // 2
    chunks = HEADS // 2
    head = features // HEADS
    bf16 = jnp.bfloat16
    f32 = jnp.float32
    anywhere = pl.BlockSpec(memory_space=pltpu.HBM)
    dma = pltpu.SemaphoreType.DMA
    return pl.pallas_call(
        pair_kernel,
        out_shape=pltpu.VMEM((1, rows, width), bf16),
        in_specs=[anywhere] * 5 + [pl.BlockSpec(memory_space=pltpu.SMEM)],
        out_specs=pl.BlockSpec(memory_space=pltpu.VMEM),
        scratch_shapes=[
            pltpu.VMEM((width, features), bf16),
            pltpu.VMEM((width, features), bf16),
            pltpu.VMEM((width, features), bf16),
            pltpu.VMEM((features, width), bf16),
            pltpu.VMEM((features, width), bf16),
            pltpu.VMEM((micro, rows, width), bf16),
            pltpu.VMEM((micro, rows, width), bf16),
            pltpu.VMEM((micro * rows, width), bf16),
            pltpu.VMEM((micro, rows, features), bf16),
            pltpu.VMEM((rows, features), bf16),
            pltpu.VMEM((rows, features), bf16),
            pltpu.VMEM((rows, features), bf16),
            pltpu.VMEM((HEADS, rows, rows), bf16),
            pltpu.VMEM((chunks + HEADS, half, head), bf16),
            pltpu.VMEM((2, HEADS, half, head), bf16),
            pltpu.VMEM((rows, features), bf16),
            pltpu.VMEM((half, features), f32),
            pltpu.VMEM((half, features), f32),
            pltpu.VMEM((half, features), f32),
            pltpu.VMEM((rows, features), f32),
            pltpu.VMEM((rows, width), f32),
            dma((3,)),
            dma((5,)),
            dma((max(2 + sum(COUNTS), 4 + 2 * max(PIECES)),)),
            pltpu.SemaphoreType.REGULAR,
        ],
        compiler_params=pltpu.CompilerParams(
            collective_id=0, has_side_effects=True, vmem_limit_bytes=62 * 1024 * 1024
        ),
        name="section_pair",
    )(inputs, w_query, w_key, w_value, w_out, mixing)


def solution(mesh):
    in_specs = (
        P("dp", None, None),
        P("section", None, None),
        P("section", None, None),
        P("section", None, None),
        P("section", None, None),
        P("section"),
    )
    out_specs = P(("dp", "section"), None, None)
    paired = mesh.shape["section"] == 2 and mesh.shape["dp"] % 8 == 0

    def either(inputs, *weights):
        square = inputs.shape[1] * HEADS == weights[2].shape[2]
        chosen = pair_body if paired and square and inputs.shape[0] == 2 else body
        return chosen(inputs, *weights)

    return jax.shard_map(either, mesh=mesh, in_specs=in_specs, out_specs=out_specs, check_vma=False)
```

```python
import functools

import jax
import jax.numpy as jnp
from jax import lax
from jax.experimental import pallas as pl
from jax.experimental.pallas import tpu as pltpu
from jax.sharding import PartitionSpec as P

HEADS = 6
THIRDS = (0, 4, 8, 12)
HALVES = (0, 6, 12)
CUTS = ((THIRDS, HALVES), (HALVES, (0, 4, 8, 10, 11, 12)))
COUNTS = [len(CUTS[n // 2][n % 2]) - 1 for n in range(4)]
PIECES = (3, 5)

epsilon = 1e-06
score_scale = 0.12
MESH = pl.DeviceIdType.MESH


def norm_rows(tensor):
    return tensor * lax.rsqrt(jnp.mean(tensor * tensor, axis=-1, keepdims=True) + epsilon)


def project(normed, weight):
    return jnp.dot(normed, weight, preferred_element_type=jnp.float32)


def kernel(
    sections,
    inputs_ref,
    wq_hbm,
    wk_hbm,
    wv_hbm,
    wo_hbm,
    mixing_ref,
    out_ref,
    wq,
    wk,
    wv,
    wo,
    h_in,
    h_out,
    v_buf,
    q_buf,
    k_buf,
    val_buf,
    p_buf,
    att_buf,
    acc_buf,
    in_sem,
    wv_sem,
    load_sem,
    hs_sem,
    hr_sem,
    vs_sem,
    vr_sem,
    os_sem,
    or_sem,
):
    me = lax.axis_index("section")
    last = sections - 1
    micro, rows, width = h_in.shape
    features = v_buf.shape[2]
    head = features // HEADS
    chunks = HEADS // 2
    span = features // chunks
    share = micro // sections
    is_first = me == 0
    is_last = me == last
    bf16 = jnp.bfloat16
    f32 = jnp.float32

    def head_part(n):
        return slice(n * head, (n + 1) * head)

    def chunk_part(j):
        return slice(j * span, (j + 1) * span)

    def input_load(i):
        return pltpu.make_async_copy(inputs_ref.at[i], h_in.at[i], in_sem.at[i])

    def value_load(j):
        return pltpu.make_async_copy(
            wv_hbm.at[0, :, chunk_part(j)], wv.at[:, chunk_part(j)], wv_sem.at[j]
        )

    loads = [
        pltpu.make_async_copy(source.at[0], target, load_sem.at[i])
        for i, (source, target) in enumerate(((wq_hbm, wq), (wk_hbm, wk), (wo_hbm, wo)))
    ]

    barrier = pltpu.get_barrier_semaphore()
    for step in range(1, sections):
        pl.semaphore_signal(
            barrier,
            inc=1,
            device_id={"section": lax.rem(me + step, sections)},
            device_id_type=MESH,
        )

    @pl.when(is_first)
    def _():
        input_load(0).start()

    for j in range(chunks):
        value_load(j).start()
    for load in loads:
        load.start()

    @pl.when(is_first)
    def _():
        for i in range(1, micro):
            input_load(i).start()

    pl.semaphore_wait(barrier, sections - 1)

    onward = jnp.minimum(me + 1, last)

    def h_copy(i):
        return pltpu.make_async_remote_copy(
            src_ref=h_out.at[i],
            dst_ref=h_in.at[i],
            send_sem=hs_sem.at[i],
            recv_sem=hr_sem.at[i],
            device_id={"section": onward},
            device_id_type=MESH,
        )

    def v_copy(i, j):
        return pltpu.make_async_remote_copy(
            src_ref=v_buf.at[i, :, chunk_part(j)],
            dst_ref=v_buf.at[i, :, chunk_part(j)],
            send_sem=vs_sem.at[i, j],
            recv_sem=vr_sem.at[i, j],
            device_id={"section": onward},
            device_id_type=MESH,
        )

    def out_copy(i):
        return pltpu.make_async_remote_copy(
            src_ref=h_out.at[i],
            dst_ref=out_ref.at[i % share],
            send_sem=os_sem.at[i],
            recv_sem=or_sem.at[i],
            device_id={"section": i // share},
            device_id_type=MESH,
        )

    row_index = lax.broadcasted_iota(jnp.int32, (rows, rows), 0)
    column_index = lax.broadcasted_iota(jnp.int32, (rows, rows), 1)
    causal = row_index >= column_index

    def fill_probabilities(normed):
        queries = project(normed, wq[...])
        key_rows = project(normed, wk[...])
        for n in range(HEADS):
            q_buf[:, head_part(n)] = norm_rows(queries[:, head_part(n)]).astype(bf16)
            k_buf[:, head_part(n)] = norm_rows(key_rows[:, head_part(n)]).astype(bf16)
        for n in range(HEADS):
            scores = (
                lax.dot_general(
                    q_buf[:, head_part(n)],
                    k_buf[:, head_part(n)],
                    (((1,), (1,)), ((), ())),
                    preferred_element_type=f32,
                )
                * score_scale
            )
            weights = jnp.where(causal, jnp.exp(scores), 0.0)
            p_buf[n] = (weights / jnp.sum(weights, axis=-1, keepdims=True)).astype(bf16)

    @pl.when(is_first)
    def _():
        def one(i, carry):
            input_load(i).wait()
            normed = norm_rows(h_in[i].astype(f32)).astype(bf16)
            for j in range(chunks):

                @pl.when(i == 0)
                def _():
                    value_load(j).wait()

                v_buf[i, :, chunk_part(j)] = project(normed, wv[:, chunk_part(j)]).astype(bf16)
                if sections > 1:

                    @pl.when(i == 0)
                    def _():
                        v_copy(i, j).start()

            @pl.when(i == 0)
            def _():
                for load in loads:
                    load.wait()

            fill_probabilities(normed)
            for n in range(HEADS):
                att_buf[:, head_part(n)] = project(p_buf[n], v_buf[i, :, head_part(n)]).astype(bf16)
            result = (h_in[i].astype(f32) + project(att_buf[...], wo[...])).astype(bf16)
            if sections > 1:
                h_out[i] = result
                h_copy(i).start()

                @pl.when(i > 0)
                def _():
                    for j in range(chunks):
                        v_copy(i, j).start()

            else:
                out_ref[i] = result
            return carry

        lax.fori_loop(0, micro, one, 0)

    if sections > 1:

        @pl.when(jnp.logical_not(is_first))
        def _():
            for j in range(chunks):
                value_load(j).wait()
            for load in loads:
                load.wait()
            mixing = mixing_ref[0]

            def one(i, carry):
                h_copy(i).wait_recv()
                normed = norm_rows(h_in[i].astype(f32)).astype(bf16)
                fill_probabilities(normed)
                val_buf[...] = mixing * project(normed, wv[...])
                for j in range(chunks):
                    v_copy(i, j).wait_recv()
                    if sections > 2:

                        @pl.when(jnp.logical_not(is_last))
                        def _():
                            v_copy(i, j).start()

                    used = (
                        val_buf[:, chunk_part(j)]
                        + (1.0 - mixing) * v_buf[i, :, chunk_part(j)].astype(f32)
                    ).astype(bf16)
                    for n in range(2):
                        att_buf[:, head_part(2 * j + n)] = project(
                            p_buf[2 * j + n], used[:, head_part(n)]
                        ).astype(bf16)
                    term = project(att_buf[:, chunk_part(j)], wo[chunk_part(j), :])
                    if j == 0:
                        acc_buf[...] = term
                    elif j < chunks - 1:
                        acc_buf[...] += term
                result = (h_in[i].astype(f32) + (acc_buf[...] + term)).astype(bf16)
                mine = jnp.logical_and(is_last, i // share == last)

                @pl.when(mine)
                def _():
                    out_ref[i % share] = result

                @pl.when(jnp.logical_not(mine))
                def _():
                    h_out[i] = result

                    @pl.when(is_last)
                    def _():
                        out_copy(i).start()

                    if sections > 2:

                        @pl.when(jnp.logical_not(is_last))
                        def _():
                            h_copy(i).start()

                return carry

            lax.fori_loop(0, micro, one, 0)

    @pl.when(jnp.logical_not(is_last))
    def _():
        for i in range(micro):
            for j in range(chunks):
                v_copy(i, j).wait_send()
            h_copy(i).wait_send()

    for i in range(micro):
        if i // share != last:

            @pl.when(is_last)
            def _():
                out_copy(i).wait_send()

            @pl.when(me == i // share)
            def _():
                out_copy(i).wait_recv()


def body(inputs, w_query, w_key, w_value, w_out, mixing):
    sections = lax.axis_size("section")
    micro, rows, width = inputs.shape
    features = w_value.shape[2]
    share = micro // sections
    bf16 = jnp.bfloat16
    anywhere = pl.BlockSpec(memory_space=pltpu.HBM)
    dma = pltpu.SemaphoreType.DMA
    return pl.pallas_call(
        functools.partial(kernel, sections),
        out_shape=pltpu.VMEM((share, rows, width), bf16),
        in_specs=[anywhere] * 5 + [pl.BlockSpec(memory_space=pltpu.SMEM)],
        out_specs=pl.BlockSpec(memory_space=pltpu.VMEM),
        scratch_shapes=[
            pltpu.VMEM((width, features), bf16),
            pltpu.VMEM((width, features), bf16),
            pltpu.VMEM((width, features), bf16),
            pltpu.VMEM((features, width), bf16),
            pltpu.VMEM((micro, rows, width), bf16),
            pltpu.VMEM((micro, rows, width), bf16),
            pltpu.VMEM((micro, rows, features), bf16),
            pltpu.VMEM((rows, features), bf16),
            pltpu.VMEM((rows, features), bf16),
            pltpu.VMEM((rows, features), jnp.float32),
            pltpu.VMEM((HEADS, rows, rows), bf16),
            pltpu.VMEM((rows, features), bf16),
            pltpu.VMEM((rows, width), jnp.float32),
            dma((micro,)),
            dma((HEADS // 2,)),
            dma((3,)),
            dma((micro,)),
            dma((micro,)),
            dma((micro, HEADS // 2)),
            dma((micro, HEADS // 2)),
            dma((micro,)),
            dma((micro,)),
        ],
        compiler_params=pltpu.CompilerParams(
            collective_id=0, has_side_effects=True, vmem_limit_bytes=62 * 1024 * 1024
        ),
        name="sections",
    )(inputs, w_query, w_key, w_value, w_out, mixing)


def pair_kernel(
    inputs_ref,
    wq_hbm,
    wk_hbm,
    wv_hbm,
    wo_hbm,
    mixing_ref,
    out_ref,
    wq,
    wk,
    wv,
    wo,
    wx,
    h_in,
    h_out,
    normed_buf,
    v_buf,
    q_buf,
    k_buf,
    used_buf,
    p_buf,
    low_buf,
    high_buf,
    att_buf,
    q_acc,
    k_acc,
    v_acc,
    val_buf,
    out_acc,
    load_sem,
    send_sem,
    recv_sem,
    met_sem,
):
    me = lax.axis_index("section")
    dp = lax.axis_index("dp")
    core = dp % 2
    across = dp + 2 - 4 * ((dp // 2) % 2)
    along = dp + 4 - 8 * ((dp // 4) % 2)
    beside = dp + 1 - 2 * core
    near = (dp // 2 + dp // 4) % 2
    most = max(PIECES)
    column = dp // 2 % 2
    mine, missed = most - 1 - column, most - 2 + column
    micro, rows, width = h_in.shape
    features = wv.shape[1]
    head = features // HEADS
    chunks = HEADS // 2
    span = features // chunks
    half = rows // 2
    share = features // 2
    piece = share // sum(PIECES)
    bf16 = jnp.bfloat16
    f32 = jnp.float32
    everything = slice(0, rows)
    early = slice(0, (chunks - 1) * span)
    late = slice((chunks - 1) * span, features)

    def head_part(n):
        return slice(n * head, (n + 1) * head)

    def chunk_part(j):
        return slice(j * span, (j + 1) * span)

    def cut_parts(i, t):
        ends = [width * n // 12 for n in CUTS[i][t]]
        return [slice(*pair) for pair in zip(ends, ends[1:])]

    def half_part(t):
        return slice(t * half, (t + 1) * half)

    def sequence_part(i):
        return slice(i * rows, (i + 1) * rows)

    def load(source, target, n):
        return pltpu.make_async_copy(source, target, n)

    def input_load(i):
        return load(inputs_ref.at[i], h_in.at[i], send_sem.at[i])

    def value_load(j):
        return load(wv_hbm.at[0, :, chunk_part(j)], wv.at[:, chunk_part(j)], load_sem.at[j])

    query_load = load(wq_hbm.at[0], wq, send_sem.at[2])
    key_load = load(wk_hbm.at[0], wk, send_sem.at[3])
    out_load = load(wo_hbm.at[0], wo, send_sem.at[4])
    values_load = load(wv_hbm.at[0], wv, load_sem.at[2])

    def share_load(r):
        part = pl.ds(pl.multiple_of((near + r) % 2 * share, share), share)
        return load(wo_hbm.at[0, part, :], wo.at[part, :], load_sem.at[r])

    def send(source, target, sent, received, device):
        return pltpu.make_async_remote_copy(
            src_ref=source,
            dst_ref=target,
            send_sem=send_sem.at[sent],
            recv_sem=recv_sem.at[received],
            device_id=device,
            device_id_type=MESH,
        )

    def cut_copy(i, t, c):
        part = (i, half_part(t), cut_parts(i, t)[c])
        place = sum(COUNTS[: 2 * i + t]) + c
        return send(h_out.at[part], h_in.at[part], 0 if i else 4, place, {"section": 1})

    def v_copy(part, n):
        return send(v_buf.at[1, :, part], v_buf.at[1, :, part], 1, sum(COUNTS) + n, {"section": 1})

    def low_copy():
        return send(low_buf, low_buf, 2, 0, {"section": 0})

    def high_copy(g):
        return send(high_buf.at[g], high_buf.at[g], 3, 1 + g, {"section": 0})

    def piece_part(far, i):
        start = (near + far) % 2 * share + core * PIECES[0] * piece + i * piece
        return pl.ds(pl.multiple_of(start, piece), piece)

    def y_copy(i):
        part = piece_part(0, i)
        sent = 1 if i else core
        return send(wo.at[part, :], wx.at[part, :], sent, 3 + i, {"section": 0})

    def side_copy(far, i):
        part = wx.at[piece_part(far, i), :]
        return send(part, part, 2, 3 + most + i, {"dp": along if i % 2 else across})

    def rare_copy():
        part = piece_part(0, mine)
        return send(wo.at[part, :], wx.at[part, :], 0, 1 + most, {"section": 0})

    def rare_side(step):
        part = wx.at[piece_part(0, mine), :]
        return send(part, part, 2, 1 + 2 * most + step, {"dp": across if step else along})

    def relay_copy():
        part = wx.at[piece_part(1, missed), :]
        return send(part, part, 2, 2 + most, {"dp": along})

    def core_copy(far, i):
        part = wx.at[piece_part(far, i), :]
        return send(part, part, 3, 3 + 2 * most, {"dp": beside})

    def pieces_wait(count, sent, received):
        part = wx.at[: count * piece, :]
        return send(part, part, sent, received, {"dp": beside})

    def rows_sent(count, sent):
        part = wx.at[:count, :]
        return send(part, part, sent, 0, {"section": 1})

    def for_core(run):
        for n in range(2):
            pl.when(core == n)(functools.partial(run, PIECES[n], PIECES[1 - n]))

    barrier = pltpu.get_barrier_semaphore()

    @pl.when(me == 1)
    def _():
        share_load(0).start()
        pl.semaphore_wait(barrier, 1)
        pl.semaphore_signal(met_sem, inc=1, device_id={"section": 0}, device_id_type=MESH)

    @pl.when(me == 0)
    def _():
        for device in ({"section": 1}, {"dp": across}, {"dp": along}, {"dp": beside}):
            pl.semaphore_signal(barrier, inc=1, device_id=device, device_id_type=MESH)

    row_index = lax.broadcasted_iota(jnp.int32, (rows, rows), 0)
    column_index = lax.broadcasted_iota(jnp.int32, (rows, rows), 1)
    causal = row_index >= column_index

    def normed_rows(values):
        return norm_rows(values.astype(f32)).astype(bf16)

    def fill_heads(target, part, values):
        for n in range(HEADS):
            target[part, head_part(n)] = norm_rows(values[:, head_part(n)]).astype(bf16)

    def probabilities(part, keys, n):
        scores = (
            lax.dot_general(
                q_buf[part, head_part(n)],
                k_buf[:keys, head_part(n)],
                (((1,), (1,)), ((), ())),
                preferred_element_type=f32,
            )
            * score_scale
        )
        weights = jnp.where(causal[part, :keys], jnp.exp(scores), 0.0)
        return weights / jnp.sum(weights, axis=-1, keepdims=True)

    @pl.when(me == 0)
    def _():
        input_load(1).start()
        value_load(0).start()
        input_load(0).start()
        for j in range(1, chunks):
            value_load(j).start()

        def fill_normed(i):
            with jax.named_scope(f"in{i}"):
                input_load(i).wait()
            normed_buf[sequence_part(i), :] = normed_rows(h_in[i])

        def fill_values(i, j):
            v_buf[i, :, chunk_part(j)] = project(
                normed_buf[sequence_part(i), :], wv[:, chunk_part(j)]
            ).astype(bf16)

        fill_normed(1)
        query_load.start()
        key_load.start()
        out_load.start()
        for j in range(chunks - 1):
            with jax.named_scope(f"wv{j}"):
                value_load(j).wait()
            fill_values(1, j)
            if j == 0:
                with jax.named_scope("met"):
                    pl.semaphore_wait(met_sem, 1)
            v_copy(chunk_part(j), 0).start()
        value_load(chunks - 1).wait()

        @pl.when(core == 0)
        def _():
            fill_values(1, chunks - 1)
            v_copy(late, 1).start()

        fill_normed(0)
        for j in range(chunks):
            fill_values(0, j)

        def fill_queries(i):
            normed = normed_buf[sequence_part(i), :]
            if i == 0:
                with jax.named_scope("wq"):
                    query_load.wait()
            fill_heads(q_buf, everything, project(normed, wq[...]))
            if i == 0:
                with jax.named_scope("wk"):
                    key_load.wait()
            fill_heads(k_buf, everything, project(normed, wk[...]))

        def attend(i, part, keys):
            for n in range(HEADS):
                p_buf[n, part, :keys] = probabilities(part, keys, n).astype(bf16)
            for n in range(HEADS):
                att_buf[part, head_part(n)] = project(
                    p_buf[n, part, :keys], v_buf[i, :keys, head_part(n)]
                ).astype(bf16)

        def next_rows(i, t):
            part = half_part(t)
            for c, columns in enumerate(cut_parts(i, t)):
                h_out[i, part, columns] = (
                    h_in[i, part, columns].astype(f32) + project(att_buf[part, :], wo[:, columns])
                ).astype(bf16)
                if (i, t) == (0, 0):
                    cut_copy(i, t, c).start()

        def start_rows(i, t):
            for c in range(COUNTS[2 * i + t]):
                cut_copy(i, t, c).start()

        def pass_on(i):
            with jax.named_scope(f"pass{i}"):
                y_copy(i).wait_recv()
            side_copy(0, i).start()
            core_copy(0, i).start()

        def pass_far(i):
            with jax.named_scope(f"far{i}"):
                side_copy(1, i).wait_recv()
            core_copy(1, i).start()

        fill_queries(0)
        for t in range(2):
            attend(0, half_part(t), (t + 1) * half)
            if t == 0:
                with jax.named_scope("wo"):
                    out_load.wait()
            with jax.named_scope(f"h0{t}"):
                next_rows(0, t)
        pl.when(core == 0)(functools.partial(start_rows, 0, 1))
        pl.when(core == 1)(functools.partial(fill_values, 1, chunks - 1))
        with jax.named_scope("bar"):
            pl.semaphore_wait(barrier, 3)

        @pl.when(core == 1)
        def _():
            with jax.named_scope("rare"):
                rare_copy().wait_recv()
            for step in range(2):
                rare_side(step).start()
            core_copy(0, mine).start()

        pl.when(core == 0)(functools.partial(pass_on, 0))
        fill_queries(1)
        attend(1, everything, rows)
        with jax.named_scope("h1"):
            for t in range(2):
                next_rows(1, t)
                pl.when(core == 0)(functools.partial(start_rows, 1, t))

        @pl.when(core == 1)
        def _():
            with jax.named_scope("yield"):
                rows_sent(half, 4).wait_send()
            start_rows(0, 1)

        pl.when(core == 1)(functools.partial(pass_on, 0))
        pass_on(1)

        @pl.when(core == 1)
        def _():
            with jax.named_scope("across"):
                rare_side(1).wait_recv()
            relay_copy().start()
            core_copy(1, missed).start()
            with jax.named_scope("along"):
                rare_side(0).wait_recv()
            core_copy(1, mine).start()

        pass_far(0)

        @pl.when(core == 1)
        def _():
            with jax.named_scope("yield"):
                rows_sent(half, 4).wait_send()
            for t in range(2):
                start_rows(1, t)
            v_copy(late, 1).start()

        for i in range(2, min(PIECES)):
            pass_on(i)
            pass_far(i - 1)

        @pl.when(core == 1)
        def _():
            with jax.named_scope("relay"):
                relay_copy().wait_recv()
            core_copy(0, missed).start()

        pass_far(min(PIECES) - 1)
        with jax.named_scope("core"):
            for_core(lambda own, other: pieces_wait(2 * other, 3, 3 + 2 * most).wait_recv())
        for t in range(2):
            part = half_part(t)
            keys = (t + 1) * half
            for n in range(HEADS):
                group, place = n // chunks, n % chunks
                if t == 0:
                    if n == 0:
                        with jax.named_scope("low"):
                            low_copy().wait_recv()
                    passed = low_buf[n // 2, :, n % 2 * half : (n % 2 + 1) * half]
                    own = low_buf[chunks + n]
                else:
                    if place == 0:
                        with jax.named_scope(f"high{group}"):
                            high_copy(group).wait_recv()
                    passed = high_buf[group, place]
                    own = high_buf[group, chunks + place]
                att_buf[part, head_part(n)] = (
                    own.astype(f32) + project(passed, v_buf[0, :keys, head_part(n)])
                ).astype(bf16)
            out_ref[0, part, :] = (
                h_out[0, part, :].astype(f32) + project(att_buf[part, :], wx[...])
            ).astype(bf16)
        with jax.named_scope("end"):
            pl.when(core == 0)(rows_sent(rows, 4).wait_send)
            rows_sent(rows, 0).wait_send()
            send(v_buf.at[1], v_buf.at[1], 1, 0, {"section": 1}).wait_send()
            for_core(lambda own, other: pieces_wait(own + own // most, 2, 0).wait_send())
            for_core(lambda own, other: pieces_wait(2 * own, 3, 0).wait_send())

    @pl.when(me == 1)
    def _():
        mixing = mixing_ref[0]
        with jax.named_scope("wo"):
            share_load(0).wait()
        pl.when(core == 1)(lambda: rare_copy().start())
        for i in range(min(PIECES)):
            y_copy(i).start()
        with jax.named_scope("y0"):
            pieces_wait(1, 0, 0).wait_send()
        query_load.start()
        key_load.start()
        values_load.start()
        share_load(1).start()
        with jax.named_scope("loads"):
            query_load.wait()
            key_load.wait()
            values_load.wait()
            share_load(1).wait()

        def fill_rows(i, t):
            part = half_part(t)
            squares = jnp.zeros((half, 1), f32)
            for c, columns in enumerate(cut_parts(i, t)):
                with jax.named_scope(f"cut{i}{t}{c}"):
                    cut_copy(i, t, c).wait_recv()
                arrived = h_in[i, part, columns]
                for target, weight in ((q_acc, wq), (k_acc, wk), (v_acc, wv)):
                    term = project(arrived, weight[columns, :])
                    if c == 0:
                        target[...] = term
                    else:
                        target[...] += term
                wide = arrived.astype(f32)
                squares += jnp.sum(wide * wide, axis=-1, keepdims=True)
            scale = lax.rsqrt(squares / width + epsilon)
            fill_heads(q_buf, part, q_acc[...] * scale)
            fill_heads(k_buf, part, k_acc[...] * scale)
            return mixing * (v_acc[...] * scale)

        for t in range(2):
            part = half_part(t)
            keys = (t + 1) * half
            used_buf[part, :] = fill_rows(0, t).astype(bf16)
            for n in range(HEADS):
                group, place = n // chunks, n % chunks
                shares = probabilities(part, keys, n)
                passed = ((1.0 - mixing) * shares).astype(bf16)
                own = project(shares.astype(bf16), used_buf[:keys, head_part(n)]).astype(bf16)
                if t == 0:
                    low_buf[n // 2, :, n % 2 * half : (n % 2 + 1) * half] = passed
                    low_buf[chunks + n] = own
                else:
                    high_buf[group, place] = passed
                    high_buf[group, chunks + place] = own
                    if place == chunks - 1:
                        high_copy(group).start()
            if t == 0:
                low_copy().start()

        def fill_used(part, columns):
            used_buf[part, columns] = (
                val_buf[part, columns] + (1.0 - mixing) * v_buf[1, part, columns].astype(f32)
            ).astype(bf16)

        def fill_attended(t, heads):
            part = half_part(t)
            keys = (t + 1) * half
            for n in heads:
                att_buf[part, head_part(n)] = project(
                    p_buf[n, part, :keys], used_buf[:keys, head_part(n)]
                ).astype(bf16)

        def finish_rows(t, columns):
            part = half_part(t)
            keys = (t + 1) * half
            for n in range(HEADS):
                p_buf[n, part, :keys] = probabilities(part, keys, n).astype(bf16)
            fill_used(part, columns)
            fill_attended(t, range(columns.stop // head))
            return h_in[1, part, :].astype(f32) + project(att_buf[part, columns], wo[columns, :])

        def finish_either(t):
            @pl.when(core == 0)
            def _():
                if t == 0:
                    v_copy(late, 1).wait_recv()
                out_ref[0, half_part(t), :] = finish_rows(t, slice(0, features)).astype(bf16)

            @pl.when(core == 1)
            def _():
                out_acc[half_part(t), :] = finish_rows(t, early)

        val_buf[half_part(0), :] = fill_rows(1, 0)
        v_copy(early, 0).wait_recv()
        finish_either(0)
        val_buf[half_part(1), :] = fill_rows(1, 1)
        with jax.named_scope("last"):
            finish_either(1)

        @pl.when(core == 1)
        def _():
            with jax.named_scope("first"):
                v_copy(late, 1).wait_recv()
            with jax.named_scope("out"):
                fill_used(everything, late)
                for t in range(2):
                    fill_attended(t, range(HEADS - 2, HEADS))
                out_ref[0] = (out_acc[...] + project(att_buf[:, late], wo[late, :])).astype(bf16)

        with jax.named_scope("end"):
            for_core(lambda own, other: pieces_wait(own - 1 - own // most, 1, 0).wait_send())
            send(low_buf, low_buf, 2, 0, {"section": 0}).wait_send()
            send(high_buf, high_buf, 3, 0, {"section": 0}).wait_send()


def pair_body(inputs, w_query, w_key, w_value, w_out, mixing):
    micro, rows, width = inputs.shape
    features = w_value.shape[2]
    half = rows // 2
    chunks = HEADS // 2
    head = features // HEADS
    bf16 = jnp.bfloat16
    f32 = jnp.float32
    anywhere = pl.BlockSpec(memory_space=pltpu.HBM)
    dma = pltpu.SemaphoreType.DMA
    return pl.pallas_call(
        pair_kernel,
        out_shape=pltpu.VMEM((1, rows, width), bf16),
        in_specs=[anywhere] * 5 + [pl.BlockSpec(memory_space=pltpu.SMEM)],
        out_specs=pl.BlockSpec(memory_space=pltpu.VMEM),
        scratch_shapes=[
            pltpu.VMEM((width, features), bf16),
            pltpu.VMEM((width, features), bf16),
            pltpu.VMEM((width, features), bf16),
            pltpu.VMEM((features, width), bf16),
            pltpu.VMEM((features, width), bf16),
            pltpu.VMEM((micro, rows, width), bf16),
            pltpu.VMEM((micro, rows, width), bf16),
            pltpu.VMEM((micro * rows, width), bf16),
            pltpu.VMEM((micro, rows, features), bf16),
            pltpu.VMEM((rows, features), bf16),
            pltpu.VMEM((rows, features), bf16),
            pltpu.VMEM((rows, features), bf16),
            pltpu.VMEM((HEADS, rows, rows), bf16),
            pltpu.VMEM((chunks + HEADS, half, head), bf16),
            pltpu.VMEM((2, HEADS, half, head), bf16),
            pltpu.VMEM((rows, features), bf16),
            pltpu.VMEM((half, features), f32),
            pltpu.VMEM((half, features), f32),
            pltpu.VMEM((half, features), f32),
            pltpu.VMEM((rows, features), f32),
            pltpu.VMEM((rows, width), f32),
            dma((3,)),
            dma((5,)),
            dma((max(2 + sum(COUNTS), 4 + 2 * max(PIECES)),)),
            pltpu.SemaphoreType.REGULAR,
        ],
        compiler_params=pltpu.CompilerParams(
            collective_id=0, has_side_effects=True, vmem_limit_bytes=62 * 1024 * 1024
        ),
        name="section_pair",
    )(inputs, w_query, w_key, w_value, w_out, mixing)


def solution(mesh):
    in_specs = (
        P("dp", None, None),
        P("section", None, None),
        P("section", None, None),
        P("section", None, None),
        P("section", None, None),
        P("section"),
    )
    out_specs = P(("dp", "section"), None, None)
    paired = mesh.shape["section"] == 2 and mesh.shape["dp"] % 8 == 0

    def either(inputs, *weights):
        square = inputs.shape[1] * HEADS == weights[2].shape[2]
        chosen = pair_body if paired and square and inputs.shape[0] == 2 else body
        return chosen(inputs, *weights)

    return jax.shard_map(either, mesh=mesh, in_specs=in_specs, out_specs=out_specs, check_vma=False)
```
